128 devices in a mesh: gen: 4 (over x_lo, core), bank: 32 (over z, y, x_hi).
Axes of the slice: x: 4 (x_hi: 2, x_lo: 2; x = x_hi * 2 + x_lo), y: 4, z: 4, core: 2. Of those that a mesh axis runs over, the one named last changes fastest.
Arguments:
- latents: bfloat16 [8192, 4096], P(('gen', 'bank')), may hold values from -6 to 6
- shift: bfloat16 [8192, 4096], P(('gen', 'bank')), may hold values from -3 to 3
- scale_mod: bfloat16 [8192, 4096], P(('gen', 'bank')), may hold values from -3 to 3
- head_weight: bfloat16 [4096, 1024], P('gen'), may hold values from -0.09375 to 0.09375
- bank: bfloat16 [65536, 1024], P('bank'), may hold values from -8 to 8
Outputs:
- update: float32 [4096, 1024], P(('gen', 'bank'))
The draws below stay inside these ranges and needn't reach their ends.
All inputs are finite; a program needn't handle non-finite values.
Results may differ from the reference program's by a relative error of at most 0.0042.
Values may be sent and summed in bfloat16 or wider, within the bound.
A program may use at most 128 MiB of HBM per device.

```python
import jax
import jax.numpy as jnp
from jax import lax

D = 4096
E = 1024
ROWS_DEV = 2048
BATCH = 2048
SAMPLES = 8192
BANK = 65536
N_GEN = 4
N_BANK = 32


def draw_bank(key, part):
    base = jax.random.fold_in(key, 7)
    key_center, key_jitter = jax.random.split(base)
    blocks = BANK // ROWS_DEV
    centers = jax.random.normal(key_center, (blocks, 1, E), jnp.float32)
    jitter = jax.random.normal(key_jitter, (blocks, ROWS_DEV, E), jnp.float32)
    drawn = jnp.clip(centers + jitter, -8.0, 8.0).reshape(BANK, E)
    return drawn.astype(jnp.bfloat16)


def block_scale(stream_key, shape, pieces, low, top_value):
    factor_of = 1.0
    for dim, blocks in pieces:
        draws = jax.random.uniform(jax.random.fold_in(jax.random.fold_in(stream_key, 6), dim), (blocks,), jnp.float32, low / len(pieces), top_value / len(pieces))
        factor_of = factor_of * jnp.repeat(jnp.exp(draws), shape[dim] // blocks).reshape((-1,) + (1,) * (len(shape) - 1 - dim))
    return factor_of


def noise(own_key, dims, scale, bound, pieces=(), kind=jnp.bfloat16):
    values = jax.random.normal(own_key, dims, jnp.float32) * scale
    if len(pieces) > 0:
        values = block_scale(own_key, dims, pieces, -0.22, 0.18) * values
    return jnp.clip(values, min=-bound, max=bound).astype(kind)


def setup_inputs(seed: int = 0) -> dict:
    arg_keys = jax.random.split(jax.random.key(seed), 6)
    latents = noise(arg_keys[0], (SAMPLES, D), 1.0, 6.0, ((0, 128),))
    shift = noise(arg_keys[1], (SAMPLES, D), 0.5, 3.0, ((0, 128),))
    scale_mod = noise(arg_keys[2], (SAMPLES, D), 0.5, 3.0, ((0, 128),))
    head_weight = noise(arg_keys[3], (D, E), D ** -0.5, 0.09375, ((0, 4),))
    bank = draw_bank(jax.random.fold_in(arg_keys[5], 71), 0)
    return {"latents": latents, "shift": shift, "scale_mod": scale_mod, "head_weight": head_weight, "bank": bank}


kernel_scale = 32.0

def reference(latents, shift, scale_mod, head_weight, bank):
    feats = latents.astype(jnp.float32)
    inverse = lax.rsqrt(lax.optimization_barrier(jnp.mean(feats * feats, axis=1, keepdims=True)) + 1e-06)
    hidden = (feats * inverse * (1.0 + scale_mod.astype(jnp.float32)) + shift.astype(jnp.float32)).astype(jnp.bfloat16)
    embed = jnp.dot(hidden, head_weight, preferred_element_type=jnp.float32)
    length = jnp.sqrt(lax.optimization_barrier(jnp.sum(embed * embed, axis=1, keepdims=True)) + 1e-06)
    unit_exact = embed / length
    unit = unit_exact.astype(jnp.bfloat16)
    bank_f = bank.astype(jnp.float32)
    bank_unit = (bank_f / jnp.sqrt(lax.optimization_barrier(jnp.sum(bank_f * bank_f, axis=1, keepdims=True)) + 1e-06)).astype(jnp.bfloat16)
    groups = unit.reshape(N_GEN, BATCH, unit.shape[1])
    diagonal = jnp.eye(BATCH, dtype=jnp.bool_)

    def batch_term(members):
        scores = jnp.dot(members, members.T, preferred_element_type=jnp.float32)
        weights = jnp.where(diagonal, jnp.float32(0.0), jnp.exp(kernel_scale * scores)).astype(jnp.bfloat16)
        return jnp.dot(weights, members, preferred_element_type=jnp.float32)
    near = lax.map(batch_term, groups).reshape(unit.shape) / (BATCH - 1)
    blocks = bank_unit.reshape(N_BANK, ROWS_DEV, bank_unit.shape[1])

    def add_block(total, block):
        scores = jnp.dot(unit, block.T, preferred_element_type=jnp.float32)
        weights = jnp.exp(kernel_scale * scores).astype(jnp.bfloat16)
        return (total + jnp.dot(weights, block, preferred_element_type=jnp.float32), None)
    total, _ = lax.scan(add_block, jnp.zeros(unit.shape, jnp.float32), blocks)
    far = total / BANK
    proof = near - far
    radial = lax.optimization_barrier(jnp.sum(unit_exact * proof, axis=1, keepdims=True))
    grad_embed = ((proof - unit_exact * radial) / length).astype(jnp.bfloat16)
    gradient = jnp.dot(hidden.T, grad_embed, preferred_element_type=jnp.float32)
    return gradient * lax.rsqrt(jnp.mean(gradient * gradient) + 1e-06)
```

```python
import functools

import jax
import jax.numpy as jnp
from jax import lax
from jax.experimental import pallas as pl
from jax.experimental.pallas import tpu as pltpu
from jax.sharding import Mesh
from jax.sharding import PartitionSpec as P

AXES = ("xl", "c", "z", "y", "xh")
MESH = pl.DeviceIdType.MESH
F32 = jnp.float32
BF16 = jnp.bfloat16
KERNEL_SCALE = 32.0
N_PLANE = 16
CHUNKS = 4
NEAREST = sorted(range(1, 16), key=lambda k: min(k // 4, 4 - k // 4) + min(k % 4, 4 - k % 4))


def kernel(
    lat, shift, scale, hw_hbm, bank_hbm, out,
    hid, lhs, w, ret, er, ue, lens, units, mate, bu, acc, wide, landed, hs, cols, grads, part, xin,
    grad, q1, q1in, q2, q2in, loc, ss, rs,
):
    xl, c, z, y, xh = (lax.axis_index(a) for a in AXES)
    me = z * 4 + y
    rows, width = ret.shape
    half = hid.shape[2]
    strip = half // 2
    brows = bu.shape[1]
    samples = acc.shape[0]

    ids = iter(range(ss.shape[0]))

    def remote(src, dst, device):
        i = next(ids)
        return pltpu.make_async_remote_copy(
            src_ref=src, dst_ref=dst, send_sem=ss.at[i], recv_sem=rs.at[i],
            device_id=device, device_id_type=MESH,
        )

    def on_plane(k):
        tz, ty = lax.rem(z + k // 4, 4), lax.rem(y + k % 4, 4)
        return {"z": tz, "y": ty}, tz * 4 + ty

    def on_line(k):
        return {
            "xl": 1 - xl if k & 1 else xl,
            "c": 1 - c if k & 2 else c,
            "xh": 1 - xh if k & 4 else xh,
        }

    core = {"c": 1 - c}
    pair = {"xl": 1 - xl}
    cut = {"xl": 1 - xl, "xh": 1 - xh}
    far_mate = {"xh": 1 - xh}

    load_w = pltpu.make_async_copy(hw_hbm, w.at[c], loc.at[0])
    load_w.start()
    load_b = pltpu.make_async_copy(bank_hbm, bu.at[0], loc.at[1])
    load_b.start()

    barrier = pltpu.get_barrier_semaphore()
    for k in range(1, N_PLANE):
        pl.semaphore_signal(barrier, inc=1, device_id=on_plane(k)[0], device_id_type=MESH)
    for k in range(1, 8):
        pl.semaphore_signal(barrier, inc=1, device_id=on_line(k), device_id_type=MESH)

    def modulate(i, _):
        r = pl.ds(pl.multiple_of(i * 16, 16), 16)
        f = lat[r, :].astype(F32)
        inverse = lax.rsqrt(jnp.mean(f * f, axis=1, keepdims=True) + 1e-06)
        h = (f * inverse * (1.0 + scale[r, :].astype(F32)) + shift[r, :].astype(F32)).astype(BF16)
        hid[0, r, :] = h[:, :half]
        hid[1, r, :] = h[:, half:]
        return 0

    lax.fori_loop(0, rows // 16, modulate, 0)
    pl.semaphore_wait(barrier, N_PLANE - 1 + 7)

    send_h = remote(hid.at[1 - xl], lhs.at[pl.ds(rows, rows)], pair)
    send_h.start()
    load_w.wait()
    send_w = remote(w.at[c], w.at[c], core)
    send_w.start()
    lhs[:rows] = hid[xl]

    load_b.wait()

    def unit_rows(i, _):
        r = pl.ds(pl.multiple_of(i * 64, 64), 64)
        b = bu[0, r, :].astype(F32)
        bu[0, r, :] = (b * lax.rsqrt(jnp.sum(b * b, axis=1, keepdims=True) + 1e-06)).astype(BF16)
        return 0

    lax.fori_loop(0, brows // 64, unit_rows, 0)
    per = brows // 2 // CHUNKS
    send_b, pass_b, pieces = [], [], []
    for i in range(CHUNKS):
        mine = pl.ds(pl.multiple_of(c * (brows // 2) + i * per, per), per)
        theirs = pl.ds(pl.multiple_of((1 - c) * (brows // 2) + i * per, per), per)
        pieces.append((mine, theirs))
        send_b.append(remote(bu.at[0, mine], bu.at[1, mine], cut))
        send_b[-1].start()
        pass_b.append(remote(bu.at[1, mine], bu.at[1, mine], core))

    send_w.wait()
    send_h.wait()
    emb = jnp.dot(lhs[...], w[...].reshape(half, width), preferred_element_type=F32)
    ret[...] = emb[rows:]
    ue[...] = emb[:rows]
    send_e = remote(ret, er, pair)
    send_e.start()
    for p in range(N_PLANE // 2):
        for g in range(4):
            o = (g % 2) * strip + p * 128
            hs[p, :, g * 128 : (g + 1) * 128] = hid[g // 2, :, o : o + 128]
    send_e.wait()
    embed = ue[...] + er[...]
    length = jnp.sqrt(jnp.sum(embed * embed, axis=1, keepdims=True) + 1e-06)
    lens[...] = length
    unit = embed / length
    ue[...] = unit
    units[me] = unit.astype(BF16)
    send_u = []
    for k in NEAREST:
        device, _ = on_plane(k)
        send_u.append(remote(units.at[me], units.at[me], device))
        send_u[-1].start()
    send_m = remote(units.at[me], mate, far_mate)
    send_m.start()
    send_c = []
    cols[me] = hs[me // 2]
    for k in NEAREST:
        device, m = on_plane(k)
        send_c.append(remote(hs.at[m // 2], cols.at[me], device))
        send_c[-1].start()
    for copy in send_u:
        copy.wait()

    tile = 256

    def weigh(slot, r, first):
        def step(i, _):
            s = pl.ds(pl.multiple_of(i * tile, tile), tile)
            u = units[pl.ds(i * (tile // rows), tile // rows)].reshape(tile, width)
            b = bu[slot, r, :]
            scores = lax.dot_general(u, b, (((1,), (1,)), ((), ())), preferred_element_type=F32)
            weight = jnp.exp(KERNEL_SCALE * scores).astype(BF16)
            total = jnp.dot(weight, b, preferred_element_type=F32)
            acc[s, :] = total if first else acc[s, :] + total
            return 0

        lax.fori_loop(0, samples // tile, step, 0)

    size = 512
    weigh(0, pl.ds(0, size), True)

    def own_rest(j, _):
        weigh(0, pl.ds(pl.multiple_of(j * size, size), size), False)
        return 0

    lax.fori_loop(1, brows // size, own_rest, 0)
    for i in range(CHUNKS):
        send_b[i].wait()
        pass_b[i].start()
        weigh(1, pieces[i][0], False)
        pass_b[i].wait()
        weigh(1, pieces[i][1], False)

    send_m.wait()
    batch = 2 * samples

    def near(i, _):
        s = pl.ds(pl.multiple_of(i * tile, tile), tile)
        u = units[pl.ds(i * (tile // rows), tile // rows)].reshape(tile, width)
        total = jnp.zeros((tile, width), F32)
        for t, own in ((units[me], True), (mate[...], False)):
            scores = lax.dot_general(u, t, (((1,), (1,)), ((), ())), preferred_element_type=F32)
            weight = jnp.exp(KERNEL_SCALE * scores)
            if own:
                row = i * tile + lax.broadcasted_iota(jnp.int32, weight.shape, 0)
                column = me * rows + lax.broadcasted_iota(jnp.int32, weight.shape, 1)
                weight = jnp.where(row == column, F32(0.0), weight)
            total = total + jnp.dot(weight.astype(BF16), t, preferred_element_type=F32)
        proof = total * (1.0 / (batch - 1)) - acc[s, :] * (1.0 / (brows * 32))
        acc[s, :] = proof
        wide[pl.ds(i * (tile // rows), tile // rows)] = proof.astype(BF16).reshape(
            tile // rows, rows, width
        )
        return 0

    lax.fori_loop(0, samples // tile, near, 0)

    send_p = []
    for k in NEAREST:
        device, m = on_plane(k)
        send_p.append(remote(wide.at[m], landed.at[k - 1], device))
        send_p[-1].start()
    proof = acc[pl.ds(pl.multiple_of(me * rows, rows), rows), :]
    for copy, k in zip(send_p, NEAREST):
        copy.wait()
        proof = proof + landed[k - 1].astype(F32)
    unit = ue[...]
    radial = jnp.sum(unit * proof, axis=1, keepdims=True)
    grads[me] = ((proof - unit * radial) / lens[...]).astype(BF16)

    send_g = []
    for k in NEAREST:
        device, _ = on_plane(k)
        send_g.append(remote(grads.at[me], grads.at[me], device))
        send_g[-1].start()
    for copy in send_c:
        copy.wait()
    for copy in send_g:
        copy.wait()

    feats = cols[...].reshape(samples, 512)
    part[...] = lax.dot_general(
        feats, grads[...].reshape(samples, width), (((0,), (0,)), ((), ())),
        preferred_element_type=F32,
    )
    lane = lax.rem(y, 2) * 64

    def block(axl, ac, axh):
        return pl.ds(pl.multiple_of((axl * 2 + ac) * 128 + lane + axh * 32, 32), 32)

    send_x = []
    for k in range(1, 8):
        to = on_line(k)
        send_x.append(remote(part.at[block(to["xl"], to["c"], to["xh"])], xin.at[k - 1], to))
        send_x[-1].start()
    total = part[block(xl, c, xh), :]
    for k in range(1, 8):
        send_x[k - 1].wait()
        total = total + xin[k - 1]
    grad[...] = total
    squares = total * total
    fold = jnp.zeros((8, 128), F32)
    for a in range(4):
        for b in range(width // 128):
            fold = fold + squares[a * 8 : a * 8 + 8, b * 128 : b * 128 + 128]
    q1[...] = fold
    send_q = []
    for k in range(1, 8):
        send_q.append(remote(q1, q1in.at[k - 1], on_line(k)))
        send_q[-1].start()
    for k in range(1, 8):
        send_q[k - 1].wait()
        fold = fold + q1in[k - 1]
    q2[...] = fold
    send_q = []
    for k in range(1, N_PLANE):
        send_q.append(remote(q2, q2in.at[k - 1], on_plane(k)[0]))
        send_q[-1].start()
    for k in range(1, N_PLANE):
        send_q[k - 1].wait()
        fold = fold + q2in[k - 1]
    mean = jnp.sum(jnp.sum(fold, axis=1, keepdims=True), axis=0, keepdims=True) / (
        4 * strip * width
    )
    out[...] = grad[...] * lax.rsqrt(mean + 1e-06)


def local(latents, shift, scale_mod, head_weight, bank):
    rows, depth = latents.shape
    width = head_weight.shape[1]
    brows = bank.shape[0]
    samples = rows * N_PLANE
    vmem = pl.BlockSpec(memory_space=pltpu.VMEM)
    hbm = pl.BlockSpec(memory_space=pl.ANY)
    n_sems = 3 + 2 * CHUNKS + 1 + 15 * 5 + 7 * 2
    return pl.pallas_call(
        kernel,
        out_shape=jax.ShapeDtypeStruct((depth // 128, width), F32),
        in_specs=[vmem, vmem, vmem, hbm, hbm],
        out_specs=vmem,
        scratch_shapes=[
            pltpu.VMEM((2, rows, depth // 2), BF16),
            pltpu.VMEM((2 * rows, depth // 2), BF16),
            pltpu.VMEM((2, depth // 4, width), BF16),
            pltpu.VMEM((rows, width), F32),
            pltpu.VMEM((rows, width), F32),
            pltpu.VMEM((rows, width), F32),
            pltpu.VMEM((rows, 1), F32),
            pltpu.VMEM((N_PLANE, rows, width), BF16),
            pltpu.VMEM((rows, width), BF16),
            pltpu.VMEM((2, brows, width), BF16),
            pltpu.VMEM((samples, width), F32),
            pltpu.VMEM((N_PLANE, rows, width), BF16),
            pltpu.VMEM((N_PLANE - 1, rows, width), BF16),
            pltpu.VMEM((N_PLANE // 2, rows, 512), BF16),
            pltpu.VMEM((N_PLANE, rows, 512), BF16),
            pltpu.VMEM((N_PLANE, rows, width), BF16),
            pltpu.VMEM((512, width), F32),
            pltpu.VMEM((7, 32, width), F32),
            pltpu.VMEM((32, width), F32),
            pltpu.VMEM((8, 128), F32),
            pltpu.VMEM((7, 8, 128), F32),
            pltpu.VMEM((8, 128), F32),
            pltpu.VMEM((15, 8, 128), F32),
            pltpu.SemaphoreType.DMA((2,)),
            pltpu.SemaphoreType.DMA((n_sems,)),
            pltpu.SemaphoreType.DMA((n_sems,)),
        ],
        compiler_params=pltpu.CompilerParams(
            collective_id=0, has_side_effects=True, vmem_limit_bytes=60 * 1024 * 1024
        ),
        name="mmd_step",
    )(latents, shift, scale_mod, head_weight, bank)


def solution(mesh):
    torus = Mesh(mesh.devices.reshape(2, 2, 4, 4, 2), AXES)
    return jax.shard_map(
        local,
        mesh=torus,
        in_specs=(P(AXES, None), P(AXES, None), P(AXES, None), P(("xl", "c"), None), P(("z", "y", "xh"), None)),
        out_specs=P(AXES, None),
        check_vma=False,
    )
```

```python
import functools

import jax
import jax.numpy as jnp
from jax import lax
from jax.experimental import pallas as pl
from jax.experimental.pallas import tpu as pltpu
from jax.sharding import Mesh
from jax.sharding import PartitionSpec as P

AXES = ("xl", "c", "z", "y", "xh")
MESH = pl.DeviceIdType.MESH
F32 = jnp.float32
BF16 = jnp.bfloat16
KERNEL_SCALE = 32.0
N_PLANE = 16
CHUNKS = 4
NEAREST = sorted(range(1, 16), key=lambda k: min(k // 4, 4 - k // 4) + min(k % 4, 4 - k % 4))


def kernel(
    lat, shift, scale, hw_hbm, bank_hbm, out,
    hid, lhs, w, ret, er, ue, lens, units, pairt, bu, acc, wide, landed, hs, cols, grads, part, mine,
    xin, grad, q1, q1in, q2, q2in, loc, ss, rs,
):
    xl, c, z, y, xh = (lax.axis_index(a) for a in AXES)
    me = z * 4 + y
    rows, width = ret.shape
    half = hid.shape[2]
    strip = half // 2
    brows = bu.shape[1] * bu.shape[2]
    quarter = bu.shape[2]
    tiles, _, trows = units.shape[:3]
    tile = N_PLANE * trows
    hrows = rows // 2

    ids = iter(range(ss.shape[0]))

    def remote(src, dst, device):
        i = next(ids)
        return pltpu.make_async_remote_copy(
            src_ref=src, dst_ref=dst, send_sem=ss.at[i], recv_sem=rs.at[i],
            device_id=device, device_id_type=MESH,
        )

    def send(src, dst, device):
        copy = remote(src, dst, device)
        copy.start()
        return copy

    def on_plane(k):
        tz, ty = lax.rem(z + k // 4, 4), lax.rem(y + k % 4, 4)
        return {"z": tz, "y": ty}, tz * 4 + ty

    def on_line(k):
        return {
            "xl": 1 - xl if k & 1 else xl,
            "c": 1 - c if k & 2 else c,
            "xh": 1 - xh if k & 4 else xh,
        }

    core = {"c": 1 - c}
    pair = {"xl": 1 - xl}
    cut = {"xl": 1 - xl, "xh": 1 - xh}
    far_mate = {"xh": 1 - xh}

    load_w = pltpu.make_async_copy(hw_hbm, w.at[c], loc.at[0])
    load_w.start()
    load_b = []
    for q in range(4):
        load_b.append(
            pltpu.make_async_copy(bank_hbm.at[pl.ds(q * quarter, quarter)], bu.at[0, q], loc.at[1 + q])
        )
        load_b[-1].start()

    barrier = pltpu.get_barrier_semaphore()
    for k in range(1, N_PLANE):
        pl.semaphore_signal(barrier, inc=1, device_id=on_plane(k)[0], device_id_type=MESH)
    for k in range(1, 8):
        pl.semaphore_signal(barrier, inc=1, device_id=on_line(k), device_id_type=MESH)

    def modulate(i, _):
        r = pl.ds(pl.multiple_of(i * 16, 16), 16)
        f = lat[r, :].astype(F32)
        inverse = lax.rsqrt(jnp.mean(f * f, axis=1, keepdims=True) + 1e-06)
        h = (f * inverse * (1.0 + scale[r, :].astype(F32)) + shift[r, :].astype(F32)).astype(BF16)
        hid[0, r, :] = h[:, :half]
        hid[1, r, :] = h[:, half:]
        return 0

    lax.fori_loop(0, rows // 16, modulate, 0)
    pl.semaphore_wait(barrier, N_PLANE - 1 + 7)

    upper, lower = pl.ds(0, hrows), pl.ds(hrows, hrows)
    send_h = [
        send(hid.at[1 - xl, upper], lhs.at[pl.ds(rows, hrows)], pair),
        send(hid.at[1 - xl, lower], lhs.at[pl.ds(rows + hrows, hrows)], cut),
    ]
    load_w.wait()
    send_w = send(w.at[c], w.at[c], core)
    lhs[:rows] = hid[xl]
    for p in range(N_PLANE // 2):
        for g in range(4):
            o = (g % 2) * strip + p * 128
            for h in range(2):
                hs[p, h, :, g * 128 : (g + 1) * 128] = hid[
                    g // 2, h * hrows : (h + 1) * hrows, o : o + 128
                ]
    send_c = []
    for k in NEAREST:
        device, m = on_plane(k)
        send_c.append(send(hs.at[m // 2], cols.at[:, me], device))
    for h in range(2):
        cols[h, me] = hs[me // 2, h]

    def unit_rows(q, lo, hi):
        def step(i, _):
            r = pl.ds(pl.multiple_of(i * 64, 64), 64)
            b = bu[0, q, r, :].astype(F32)
            bu[0, q, r, :] = (b * lax.rsqrt(jnp.sum(b * b, axis=1, keepdims=True) + 1e-06)).astype(BF16)
            return 0

        lax.fori_loop(lo // 64, hi // 64, step, 0)

    for q in range(4):
        load_b[q].wait()
    gone = (1 - xl) * 2 + c
    own_q = xl * 2 + c
    pair_q = (1 - xl) * 2 + c
    per = quarter // CHUNKS

    def piece(i):
        return pl.ds(i * per, per)

    send_b = [remote(bu.at[0, gone, piece(i)], bu.at[1, gone, piece(i)], cut) for i in range(CHUNKS)]
    pass_core = [remote(bu.at[1, own_q, piece(i)], bu.at[1, own_q, piece(i)], core) for i in range(CHUNKS)]
    pass_pair = [remote(bu.at[1, own_q, piece(i)], bu.at[1, own_q, piece(i)], pair) for i in range(CHUNKS)]
    pass_last = [remote(bu.at[1, pair_q, piece(i)], bu.at[1, pair_q, piece(i)], core) for i in range(CHUNKS)]
    unit_rows(gone, 0, quarter)
    send_b[0].start()
    for k in range(1, 4):
        unit_rows(lax.rem(gone + k, 4), 0, quarter)

    send_w.wait()
    for copy in send_h:
        copy.wait()
    emb = jnp.dot(lhs[...], w[...].reshape(half, width), preferred_element_type=F32)
    ret[...] = emb[rows:]
    ue[...] = emb[:rows]
    send_e = [
        send(ret.at[upper], er.at[upper], pair),
        send(ret.at[lower], er.at[lower], cut),
    ]
    for i in range(1, CHUNKS):
        send_b[i].start()
    for copy in send_e:
        copy.wait()
    embed = ue[...] + er[...]
    length = jnp.sqrt(jnp.sum(embed * embed, axis=1, keepdims=True) + 1e-06)
    lens[...] = length
    unit = embed / length
    ue[...] = unit
    unit_b = unit.astype(BF16)
    pairt[:rows] = unit_b
    for j in range(tiles):
        units[j, me] = unit_b[j * trows : (j + 1) * trows]
    send_u = [
        [send(units.at[j, me], units.at[j, me], on_plane(k)[0]) for k in NEAREST] for j in range(tiles)
    ]
    send_m = send(pairt.at[pl.ds(0, rows)], pairt.at[pl.ds(rows, rows)], far_mate)

    def pass_on(i):
        send_b[i].wait()
        pass_core[i].start()
        pass_pair[i].start()

    def pass_again(i):
        pass_pair[i].wait()
        pass_last[i].start()

    def weigh(slot, j, order, first):
        u = units[j].reshape(tile, width)
        total = None if first else acc[j]
        for q in order:
            b = bu[slot, q]
            scores = lax.dot_general(u, b, (((1,), (1,)), ((), ())), preferred_element_type=F32)
            weight = jnp.exp(KERNEL_SCALE * scores).astype(BF16)
            term = jnp.dot(weight, b, preferred_element_type=F32)
            total = term if total is None else total + term
        acc[j] = total

    batch = 2 * tiles * tile

    def finish(j):
        u = units[j].reshape(tile, width)
        t = pairt[...]
        scores = lax.dot_general(u, t, (((1,), (1,)), ((), ())), preferred_element_type=F32)
        row = lax.broadcasted_iota(jnp.int32, scores.shape, 0) - me * trows
        column = lax.broadcasted_iota(jnp.int32, scores.shape, 1) - j * trows
        same = jnp.logical_and(row == column, jnp.logical_and(column >= 0, column < trows))
        weight = jnp.where(same, F32(0.0), jnp.exp(KERNEL_SCALE * scores)).astype(BF16)
        total = jnp.dot(weight, t, preferred_element_type=F32)
        proof = total * (1.0 / (batch - 1)) - acc[j] * (1.0 / (brows * 32))
        acc[j] = proof
        wide[j] = proof.astype(BF16).reshape(N_PLANE, trows, width)
        sends = []
        for k in NEAREST:
            device, m = on_plane(k)
            sends.append(send(wide.at[j, m], landed.at[j, k - 1], device))
        return sends

    own = (0, 1, 2, 3)
    other = (own_q, xl * 2 + 1 - c, pair_q, (1 - xl) * 2 + 1 - c)
    pass_on(0)
    pass_on(1)
    for copy in send_u[0]:
        copy.wait()
    weigh(0, 0, own, True)
    pass_on(2)
    pass_again(0)
    for copy in send_u[1]:
        copy.wait()
    weigh(0, 1, own, True)
    pass_on(3)
    pass_again(1)
    for copy in send_u[2]:
        copy.wait()
    weigh(0, 2, own, True)
    pass_again(2)
    pass_again(3)
    for i in range(CHUNKS):
        pass_core[i].wait()
    for i in range(CHUNKS):
        pass_last[i].wait()
    weigh(1, 0, other, False)
    send_m.wait()
    send_p = [finish(0)]
    weigh(1, 1, other, False)
    send_p.append(finish(1))
    weigh(1, 2, other, False)
    send_p.append(finish(2))
    for copy in send_u[3]:
        copy.wait()
    weigh(0, 3, own, True)
    weigh(1, 3, other, False)
    send_p.append(finish(3))

    for j in range(tiles):
        proof = acc[j, pl.ds(pl.multiple_of(me * trows, trows), trows), :]
        for copy, k in zip(send_p[j], NEAREST):
            copy.wait()
            proof = proof + landed[j, k - 1].astype(F32)
        r = slice(j * trows, (j + 1) * trows)
        unit = ue[r, :]
        radial = jnp.sum(unit * proof, axis=1, keepdims=True)
        o = (j * trows) % hrows
        grads[j * trows // hrows, me, o : o + trows, :] = (
            (proof - unit * radial) / lens[r, :]
        ).astype(BF16)

    def along(h, second, d):
        if (h == 0) != second:
            return {"z": lax.rem(z + d, 4)}
        return {"y": lax.rem(y + d, 4)}

    def source(h, d):
        if h == 0:
            return lax.rem(z + 4 - d, 4) * 4 + y
        return z * 4 + lax.rem(y + 4 - d, 4)

    steps = (1, 3, 2)
    first = {}
    for d in steps:
        for h in range(2):
            first[h, d] = send(grads.at[h, me], grads.at[h, me], along(h, False, d))
    second = []
    for d in steps:
        for h in range(2):
            second.append(send(grads.at[h, me], grads.at[h, me], along(h, True, d)))
    for d in steps:
        for h in range(2):
            first[h, d].wait()
            m = source(h, d)
            for e in steps:
                second.append(send(grads.at[h, m], grads.at[h, m], along(h, True, e)))
    for copy in send_c:
        copy.wait()
    for copy in second:
        copy.wait()

    feats = cols[...].reshape(N_PLANE * rows, 512)
    part[...] = lax.dot_general(
        feats, grads[...].reshape(N_PLANE * rows, width), (((0,), (0,)), ((), ())),
        preferred_element_type=F32,
    )
    lane = lax.rem(y, 2) * 64

    def strip_of(axl, ac):
        return pl.ds(pl.multiple_of((axl * 2 + ac) * 128 + lane, 64), 64)

    swap = [send(part.at[strip_of(a, 1 - c)], mine.at[a], core) for a in range(2)]
    for a in range(2):
        swap[a].wait()
        mine[2 + a] = mine[a] + part[strip_of(a, c), :]
    send_x = []
    for k in (1, 5, 4):
        to = on_line(k)
        block = mine.at[2 + to["xl"], pl.ds(pl.multiple_of(to["xh"] * 32, 32), 32)]
        send_x.append(send(block, xin.at[len(send_x)], to))
    total = mine[2 + xl, pl.ds(pl.multiple_of(xh * 32, 32), 32), :]
    for i in range(3):
        send_x[i].wait()
        total = total + xin[i]
    grad[...] = total
    squares = total * total
    fold = jnp.zeros((8, 128), F32)
    for a in range(4):
        for b in range(width // 128):
            fold = fold + squares[a * 8 : a * 8 + 8, b * 128 : b * 128 + 128]
    q1[...] = fold
    send_q = []
    for k in range(1, 8):
        send_q.append(send(q1, q1in.at[k - 1], on_line(k)))
    for k in range(1, 8):
        send_q[k - 1].wait()
        fold = fold + q1in[k - 1]
    q2[...] = fold
    send_q = []
    for k in range(1, N_PLANE):
        send_q.append(send(q2, q2in.at[k - 1], on_plane(k)[0]))
    for k in range(1, N_PLANE):
        send_q[k - 1].wait()
        fold = fold + q2in[k - 1]
    mean = jnp.sum(jnp.sum(fold, axis=1, keepdims=True), axis=0, keepdims=True) / (
        4 * strip * width
    )
    out[...] = grad[...] * lax.rsqrt(mean + 1e-06)


def local(latents, shift, scale_mod, head_weight, bank):
    rows, depth = latents.shape
    width = head_weight.shape[1]
    brows = bank.shape[0]
    vmem = pl.BlockSpec(memory_space=pltpu.VMEM)
    hbm = pl.BlockSpec(memory_space=pl.ANY)
    n_sems = 5 + 4 * CHUNKS + 15 + 60 + 1 + 60 + 30 + 5 + 7 + 15
    return pl.pallas_call(
        kernel,
        out_shape=jax.ShapeDtypeStruct((depth // 128, width), F32),
        in_specs=[vmem, vmem, vmem, hbm, hbm],
        out_specs=vmem,
        scratch_shapes=[
            pltpu.VMEM((2, rows, depth // 2), BF16),
            pltpu.VMEM((2 * rows, depth // 2), BF16),
            pltpu.VMEM((2, depth // 4, width), BF16),
            pltpu.VMEM((rows, width), F32),
            pltpu.VMEM((rows, width), F32),
            pltpu.VMEM((rows, width), F32),
            pltpu.VMEM((rows, 1), F32),
            pltpu.VMEM((4, N_PLANE, rows // 4, width), BF16),
            pltpu.VMEM((2 * rows, width), BF16),
            pltpu.VMEM((2, 4, brows // 4, width), BF16),
            pltpu.VMEM((4, N_PLANE * rows // 4, width), F32),
            pltpu.VMEM((4, N_PLANE, rows // 4, width), BF16),
            pltpu.VMEM((4, N_PLANE - 1, rows // 4, width), BF16),
            pltpu.VMEM((N_PLANE // 2, 2, rows // 2, 512), BF16),
            pltpu.VMEM((2, N_PLANE, rows // 2, 512), BF16),
            pltpu.VMEM((2, N_PLANE, rows // 2, width), BF16),
            pltpu.VMEM((512, width), F32),
            pltpu.VMEM((4, 64, width), F32),
            pltpu.VMEM((3, 32, width), F32),
            pltpu.VMEM((32, width), F32),
            pltpu.VMEM((8, 128), F32),
            pltpu.VMEM((7, 8, 128), F32),
            pltpu.VMEM((8, 128), F32),
            pltpu.VMEM((15, 8, 128), F32),
            pltpu.SemaphoreType.DMA((5,)),
            pltpu.SemaphoreType.DMA((n_sems,)),
            pltpu.SemaphoreType.DMA((n_sems,)),
        ],
        compiler_params=pltpu.CompilerParams(
            collective_id=0, has_side_effects=True, vmem_limit_bytes=60 * 1024 * 1024
        ),
        name="mmd_step",
    )(latents, shift, scale_mod, head_weight, bank)


def solution(mesh):
    torus = Mesh(mesh.devices.reshape(2, 2, 4, 4, 2), AXES)
    return jax.shard_map(
        local,
        mesh=torus,
        in_specs=(P(AXES, None), P(AXES, None), P(AXES, None), P(("xl", "c"), None), P(("z", "y", "xh"), None)),
        out_specs=P(AXES, None),
        check_vma=False,
    )
```

```python
import functools

import jax
import jax.numpy as jnp
from jax import lax
from jax.experimental import pallas as pl
from jax.experimental.pallas import tpu as pltpu
from jax.sharding import Mesh
from jax.sharding import PartitionSpec as P

AXES = ("xl", "c", "z", "y", "xh")
MESH = pl.DeviceIdType.MESH
F32 = jnp.float32
BF16 = jnp.bfloat16
KERNEL_SCALE = 32.0
N_PLANE = 16
CHUNKS = 8
NEAREST = sorted(range(1, 16), key=lambda k: min(k // 4, 4 - k // 4) + min(k % 4, 4 - k % 4))


def kernel(
    lat, shift, scale, hw_hbm, bank_hbm, grad, factor,
    hid, lhs, w, ret, er, ue, lens, units, pairt, bu, acc, wide, landed, mids, landed2, keep, hs, cols, grads, part, mine,
    xin, q1, q1in, q2, q2in, loc, ss, rs,
):
    xl, c, z, y, xh = (lax.axis_index(a) for a in AXES)
    me = z * 4 + y
    rows, width = ret.shape
    half = hid.shape[2]
    strip = half // 2
    brows = bu.shape[1] * bu.shape[2]
    quarter = bu.shape[2]
    tiles, _, trows = units.shape[:3]
    tile = N_PLANE * trows
    hrows = rows // 2

    ids = iter(range(ss.shape[0]))

    def remote(src, dst, device):
        i = next(ids)
        return pltpu.make_async_remote_copy(
            src_ref=src, dst_ref=dst, send_sem=ss.at[i], recv_sem=rs.at[i],
            device_id=device, device_id_type=MESH,
        )

    def send(src, dst, device):
        copy = remote(src, dst, device)
        copy.start()
        return copy

    def on_plane(k):
        tz, ty = lax.rem(z + k // 4, 4), lax.rem(y + k % 4, 4)
        return {"z": tz, "y": ty}, tz * 4 + ty

    def on_line(k):
        return {
            "xl": 1 - xl if k & 1 else xl,
            "c": 1 - c if k & 2 else c,
            "xh": 1 - xh if k & 4 else xh,
        }

    core = {"c": 1 - c}
    pair = {"xl": 1 - xl}
    cut = {"xl": 1 - xl, "xh": 1 - xh}
    far_mate = {"xh": 1 - xh}

    gone = (1 - xl) * 2 + c
    load_b = []
    for k in range(4):
        q = lax.rem(gone + k, 4)
        rows_q = pl.ds(pl.multiple_of(q * quarter, quarter), quarter)
        load_b.append(pltpu.make_async_copy(bank_hbm.at[rows_q], bu.at[0, q], loc.at[1 + k]))
    load_w = pltpu.make_async_copy(hw_hbm, w.at[c], loc.at[0])
    load_b[0].start()
    load_w.start()
    for k in range(1, 4):
        load_b[k].start()

    barrier = pltpu.get_barrier_semaphore()
    for k in range(1, N_PLANE):
        pl.semaphore_signal(barrier, inc=1, device_id=on_plane(k)[0], device_id_type=MESH)
    for k in range(1, 8):
        pl.semaphore_signal(barrier, inc=1, device_id=on_line(k), device_id_type=MESH)

    def modulate(i, _):
        r = pl.ds(pl.multiple_of(i * 16, 16), 16)
        f = lat[r, :].astype(F32)
        inverse = lax.rsqrt(jnp.mean(f * f, axis=1, keepdims=True) + 1e-06)
        h = (f * inverse * (1.0 + scale[r, :].astype(F32)) + shift[r, :].astype(F32)).astype(BF16)
        hid[0, r, :] = h[:, :half]
        hid[1, r, :] = h[:, half:]
        return 0

    lax.fori_loop(0, rows // 16, modulate, 0)
    for p in range(N_PLANE // 2):
        for g in range(4):
            o = (g % 2) * strip + p * 128
            for j in range(tiles):
                hs[p, j, :, g * 128 : (g + 1) * 128] = hid[
                    g // 2, j * trows : (j + 1) * trows, o : o + 128
                ]
    for j in range(tiles):
        cols[j, me] = hs[me // 2, j]
    lhs[:rows] = hid[xl]

    def unit_rows(q):
        def step(i, _):
            r = pl.ds(pl.multiple_of(i * 64, 64), 64)
            b = bu[0, q, r, :].astype(F32)
            bu[0, q, r, :] = (b * lax.rsqrt(jnp.sum(b * b, axis=1, keepdims=True) + 1e-06)).astype(BF16)
            return 0

        lax.fori_loop(0, quarter // 64, step, 0)

    load_b[0].wait()
    own_q = xl * 2 + c
    pair_q = (1 - xl) * 2 + c
    per = quarter // CHUNKS
    unit_rows(gone)
    pl.semaphore_wait(barrier, N_PLANE - 1 + 7)

    upper, lower = pl.ds(0, hrows), pl.ds(hrows, hrows)
    send_h = [
        send(hid.at[1 - xl, upper], lhs.at[pl.ds(rows, hrows)], pair),
        send(hid.at[1 - xl, lower], lhs.at[pl.ds(rows + hrows, hrows)], cut),
    ]
    load_w.wait()
    send_w = send(w.at[c], w.at[c], core)

    def piece(i):
        return pl.ds(i * per, per)

    send_b = [remote(bu.at[0, gone, piece(i)], bu.at[1, gone, piece(i)], cut) for i in range(CHUNKS)]
    pass_core = [remote(bu.at[1, own_q, piece(i)], bu.at[1, own_q, piece(i)], core) for i in range(CHUNKS)]
    pass_pair = [remote(bu.at[1, own_q, piece(i)], bu.at[1, own_q, piece(i)], pair) for i in range(CHUNKS)]
    pass_last = [remote(bu.at[1, pair_q, piece(i)], bu.at[1, pair_q, piece(i)], core) for i in range(CHUNKS)]
    send_b[0].start()
    send_c = []
    for k in NEAREST:
        device, m = on_plane(k)
        send_c.append(send(hs.at[m // 2], cols.at[:, me], device))
    for k in range(1, 4):
        load_b[k].wait()
        unit_rows(lax.rem(gone + k, 4))

    send_w.wait()
    for copy in send_h:
        copy.wait()
    emb = jnp.dot(lhs[...], w[...].reshape(half, width), preferred_element_type=F32)
    ret[...] = emb[rows:]
    ue[...] = emb[:rows]
    send_e = [
        send(ret.at[upper], er.at[upper], pair),
        send(ret.at[lower], er.at[lower], cut),
    ]
    for i in range(1, CHUNKS):
        send_b[i].start()
    for copy in send_e:
        copy.wait()
    embed = ue[...] + er[...]
    length = jnp.sqrt(jnp.sum(embed * embed, axis=1, keepdims=True) + 1e-06)
    lens[...] = length
    unit = embed / length
    ue[...] = unit
    unit_b = unit.astype(BF16)
    pairt[:rows] = unit_b
    for j in range(tiles):
        units[j, me] = unit_b[j * trows : (j + 1) * trows]

    def along(h, second, d):
        if (h == 0) != second:
            return {"z": lax.rem(z + d, 4)}
        return {"y": lax.rem(y + d, 4)}

    def source(h, d):
        if h == 0:
            return lax.rem(z + 4 - d, 4) * 4 + y
        return z * 4 + lax.rem(y + 4 - d, 4)

    steps = (1, 3, 2)

    def gather(block):
        first, second = {}, []
        for d in steps:
            for h in range(2):
                first[h, d] = send(block(h, me), block(h, me), along(h, False, d))
        for d in steps:
            for h in range(2):
                second.append(send(block(h, me), block(h, me), along(h, True, d)))

        def forward():
            for d in steps:
                for h in range(2):
                    first[h, d].wait()
                    m = source(h, d)
                    for e in steps:
                        second.append(send(block(h, m), block(h, m), along(h, True, e)))

        def done():
            for copy in second:
                copy.wait()

        return forward, done

    def gather_units(j):
        return gather(lambda h, m: units.at[j, m, :, pl.ds(h * (width // 2), width // 2)])

    flows = [gather_units(0), gather_units(1)]

    def pass_on(i):
        send_b[i].wait()
        pass_core[i].start()
        pass_pair[i].start()

    def pass_again(i):
        pass_pair[i].wait()
        pass_last[i].start()

    def weigh(slot, j, order, first):
        u = units[j].reshape(tile, width)
        total = None if first else acc[j].reshape(tile, width)
        for q in order:
            b = bu[slot, q]
            scores = lax.dot_general(u, b, (((1,), (1,)), ((), ())), preferred_element_type=F32)
            weight = jnp.exp(KERNEL_SCALE * scores).astype(BF16)
            term = jnp.dot(weight, b, preferred_element_type=F32)
            total = term if total is None else total + term
        acc[j] = total.reshape(4, 4, trows, width)

    batch = 2 * tiles * tile

    def finish(j):
        u = units[j].reshape(tile, width)
        t = pairt[...]
        scores = lax.dot_general(u, t, (((1,), (1,)), ((), ())), preferred_element_type=F32)
        row = lax.broadcasted_iota(jnp.int32, scores.shape, 0) - me * trows
        column = lax.broadcasted_iota(jnp.int32, scores.shape, 1) - j * trows
        same = jnp.logical_and(row == column, jnp.logical_and(column >= 0, column < trows))
        weight = jnp.where(same, F32(0.0), jnp.exp(KERNEL_SCALE * scores)).astype(BF16)
        total = jnp.dot(weight, t, preferred_element_type=F32)
        proof = total * (1.0 / (batch - 1)) - acc[j].reshape(tile, width) * (1.0 / (brows * 32))
        proof = proof.reshape(4, 4, trows, width)
        acc[j] = proof
        wide[j] = proof.astype(BF16)
        sends = {}
        for d in steps:
            tz, ty = lax.rem(z + d, 4), lax.rem(y + d, 4)
            sends[0, d] = send(wide.at[j, tz, :, :, left], landed.at[j, 0, d - 1], {"z": tz})
            sends[1, d] = send(wide.at[j, :, ty, :, right], landed.at[j, 1, d - 1], {"y": ty})
        return sends

    left, right = pl.ds(0, width // 2), pl.ds(width // 2, width // 2)

    def middle(j, firsts):
        sends = []
        for h in range(2):
            part_sum = acc[j, z, :, :, left] if h == 0 else acc[j, :, y, :, right]
            for d in steps:
                firsts[h, d].wait()
                part_sum = part_sum + landed[j, h, d - 1].astype(F32)
            keep[...] = part_sum
            mids[j, h] = part_sum.astype(BF16)
            acc[j, 0, h, :, left] = keep[y if h == 0 else z]
            for e in steps:
                to = lax.rem((y if h == 0 else z) + e, 4)
                sends.append(
                    send(mids.at[j, h, to], landed2.at[j, h, e - 1], {"y": to} if h == 0 else {"z": to})
                )
        return sends

    def land(j, sends):
        for copy in sends:
            copy.wait()
        halves = []
        for h in range(2):
            own_sum = acc[j, 0, h, :, left]
            for e in steps:
                own_sum = own_sum + landed2[j, h, e - 1].astype(F32)
            halves.append(own_sum)
        proof = jnp.concatenate(halves, axis=1)
        r = slice(j * trows, (j + 1) * trows)
        unit = ue[r, :]
        radial = jnp.sum(unit * proof, axis=1, keepdims=True)
        grads[j, me] = ((proof - unit * radial) / lens[r, :]).astype(BF16)
        return gather(lambda h, m: grads.at[j, m, :, pl.ds(h * (width // 2), width // 2)])

    own = (0, 1, 2, 3)
    core_q = xl * 2 + 1 - c
    near_q = (own_q, core_q)
    late_q = (pair_q, (1 - xl) * 2 + 1 - c)
    pass_on(0)
    flows[0][0]()
    flows.append(gather_units(2))
    pass_on(1)
    flows[1][0]()
    flows.append(gather_units(3))
    pass_on(2)
    flows[0][1]()
    pass_on(3)
    weigh(0, 0, own, True)
    flows[2][0]()
    pass_on(4)
    pass_again(0)
    pass_again(1)
    flows[1][1]()
    weigh(0, 1, own, True)
    flows[3][0]()
    pass_on(5)
    pass_again(2)
    flows[2][1]()
    weigh(0, 2, own, True)
    pass_on(6)
    pass_again(3)
    flows[3][1]()
    weigh(0, 3, own, True)
    pass_on(7)
    send_m = send(pairt.at[pl.ds(0, rows)], pairt.at[pl.ds(rows, rows)], far_mate)
    pass_again(4)
    weigh(1, 2, (own_q,), False)
    weigh(1, 3, (own_q,), False)
    pass_again(5)
    for i in range(CHUNKS):
        pass_core[i].wait()
    weigh(1, 0, near_q, False)
    pass_again(6)
    weigh(1, 1, near_q, False)
    weigh(1, 2, (core_q,), False)
    weigh(1, 3, (core_q,), False)
    pass_again(7)
    for i in range(CHUNKS):
        pass_last[i].wait()
    send_m.wait()
    weigh(1, 0, late_q, False)
    send_p = [finish(0)]
    weigh(1, 1, late_q, False)
    send_p.append(finish(1))
    weigh(1, 2, late_q, False)
    send_p.append(finish(2))
    middles = [middle(0, send_p[0])]
    weigh(1, 3, late_q, False)
    send_p.append(finish(3))
    middles.append(middle(1, send_p[1]))
    spread = [land(0, middles[0])]
    middles.append(middle(2, send_p[2]))
    spread.append(land(1, middles[1]))
    middles.append(middle(3, send_p[3]))
    spread[0][0]()
    spread.append(land(2, middles[2]))
    spread[1][0]()
    spread.append(land(3, middles[3]))
    spread[2][0]()
    spread[3][0]()
    for copy in send_c:
        copy.wait()
    for j in range(tiles):
        spread[j][1]()

    feats = cols[...].reshape(N_PLANE * rows, 512)
    part[...] = lax.dot_general(
        feats, grads[...].reshape(N_PLANE * rows, width), (((0,), (0,)), ((), ())),
        preferred_element_type=F32,
    )
    lane = lax.rem(y, 2) * 64

    def strip_of(axl, ac):
        return pl.ds(pl.multiple_of((axl * 2 + ac) * 128 + lane, 64), 64)

    swap = [send(part.at[strip_of(a, 1 - c)], mine.at[a], core) for a in range(2)]
    for a in range(2):
        swap[a].wait()
        mine[2 + a] = mine[a] + part[strip_of(a, c), :]
    send_x = []
    for k in (1, 5, 4):
        to = on_line(k)
        block = mine.at[2 + to["xl"], pl.ds(pl.multiple_of(to["xh"] * 32, 32), 32)]
        send_x.append(send(block, xin.at[len(send_x)], to))
    total = mine[2 + xl, pl.ds(pl.multiple_of(xh * 32, 32), 32), :]
    for i in range(3):
        send_x[i].wait()
        total = total + xin[i]
    grad[...] = total
    squares = total * total
    fold = jnp.zeros((8, 128), F32)
    for a in range(4):
        for b in range(width // 128):
            fold = fold + squares[a * 8 : a * 8 + 8, b * 128 : b * 128 + 128]
    q1[...] = fold
    send_q = []
    for k in range(1, 8):
        send_q.append(send(q1, q1in.at[k - 1], on_line(k)))
    for k in range(1, 8):
        send_q[k - 1].wait()
        fold = fold + q1in[k - 1]
    q2[...] = fold
    send_q = []
    for k in range(1, N_PLANE):
        send_q.append(send(q2, q2in.at[k - 1], on_plane(k)[0]))
    for k in range(1, N_PLANE):
        send_q[k - 1].wait()
        fold = fold + q2in[k - 1]
    mean = jnp.sum(jnp.sum(fold, axis=1, keepdims=True), axis=0, keepdims=True) / (
        4 * strip * width
    )
    factor[...] = jnp.broadcast_to(lax.rsqrt(mean + 1e-06), factor.shape)


def local(latents, shift, scale_mod, head_weight, bank):
    rows, depth = latents.shape
    width = head_weight.shape[1]
    brows = bank.shape[0]
    vmem = pl.BlockSpec(memory_space=pltpu.VMEM)
    hbm = pl.BlockSpec(memory_space=pl.ANY)
    n_sems = 5 + 4 * CHUNKS + 15 + 4 * 30 + 1 + 4 * 12 + 4 * 30 + 5 + 7 + 15
    gradient, factor = pl.pallas_call(
        kernel,
        out_shape=(
            jax.ShapeDtypeStruct((depth // 128, width), F32),
            jax.ShapeDtypeStruct((1, 128), F32),
        ),
        in_specs=[vmem, vmem, vmem, hbm, hbm],
        out_specs=(vmem, vmem),
        scratch_shapes=[
            pltpu.VMEM((2, rows, depth // 2), BF16),
            pltpu.VMEM((2 * rows, depth // 2), BF16),
            pltpu.VMEM((2, depth // 4, width), BF16),
            pltpu.VMEM((rows, width), F32),
            pltpu.VMEM((rows, width), F32),
            pltpu.VMEM((rows, width), F32),
            pltpu.VMEM((rows, 1), F32),
            pltpu.VMEM((4, N_PLANE, rows // 4, width), BF16),
            pltpu.VMEM((2 * rows, width), BF16),
            pltpu.VMEM((2, 4, brows // 4, width), BF16),
            pltpu.VMEM((4, 4, 4, rows // 4, width), F32),
            pltpu.VMEM((4, 4, 4, rows // 4, width), BF16),
            pltpu.VMEM((4, 2, 3, 4, rows // 4, width // 2), BF16),
            pltpu.VMEM((4, 2, 4, rows // 4, width // 2), BF16),
            pltpu.VMEM((4, 2, 3, rows // 4, width // 2), BF16),
            pltpu.VMEM((4, rows // 4, width // 2), F32),
            pltpu.VMEM((N_PLANE // 2, 4, rows // 4, 512), BF16),
            pltpu.VMEM((4, N_PLANE, rows // 4, 512), BF16),
            pltpu.VMEM((4, N_PLANE, rows // 4, width), BF16),
            pltpu.VMEM((512, width), F32),
            pltpu.VMEM((4, 64, width), F32),
            pltpu.VMEM((3, 32, width), F32),
            pltpu.VMEM((8, 128), F32),
            pltpu.VMEM((7, 8, 128), F32),
            pltpu.VMEM((8, 128), F32),
            pltpu.VMEM((15, 8, 128), F32),
            pltpu.SemaphoreType.DMA((5,)),
            pltpu.SemaphoreType.DMA((n_sems,)),
            pltpu.SemaphoreType.DMA((n_sems,)),
        ],
        compiler_params=pltpu.CompilerParams(
            collective_id=0, has_side_effects=True, vmem_limit_bytes=60 * 1024 * 1024
        ),
        name="mmd_step",
    )(latents, shift, scale_mod, head_weight, bank)
    return gradient * factor[0, 0]


def solution(mesh):
    torus = Mesh(mesh.devices.reshape(2, 2, 4, 4, 2), AXES)
    return jax.shard_map(
        local,
        mesh=torus,
        in_specs=(P(AXES, None), P(AXES, None), P(AXES, None), P(("xl", "c"), None), P(("z", "y", "xh"), None)),
        out_specs=P(AXES, None),
        check_vma=False,
    )
```

```python
import functools

import jax
import jax.numpy as jnp
from jax import lax
from jax.experimental import pallas as pl
from jax.experimental.pallas import tpu as pltpu
from jax.sharding import Mesh
from jax.sharding import PartitionSpec as P

AXES = ("xl", "c", "z", "y", "xh")
MESH = pl.DeviceIdType.MESH
F32 = jnp.float32
BF16 = jnp.bfloat16
KERNEL_SCALE = 32.0
N_PLANE = 16
CHUNKS = 8
NEAREST = sorted(range(1, 16), key=lambda k: min(k // 4, 4 - k // 4) + min(k % 4, 4 - k % 4))


def kernel(
    lat, shift, scale, hw_hbm, bank_hbm, grad, factor,
    hid, lhs, w, ret, er, ue, lens, units, pairt, bu, acc, wide, landed, mids, landed2, keep, hs, cols, grads, part, mine,
    xin, xout, q1, q1in, q2, q2in, loc, ss, rs,
):
    xl, c, z, y, xh = (lax.axis_index(a) for a in AXES)
    me = z * 4 + y
    rows, width = ret.shape
    half = hid.shape[2]
    strip = half // 2
    brows = bu.shape[1] * bu.shape[2]
    quarter = bu.shape[2]
    tiles, _, trows = units.shape[:3]
    tile = N_PLANE * trows
    hrows = rows // 2

    ids = iter(range(ss.shape[0]))

    def remote(src, dst, device):
        i = next(ids)
        return pltpu.make_async_remote_copy(
            src_ref=src, dst_ref=dst, send_sem=ss.at[i], recv_sem=rs.at[i],
            device_id=device, device_id_type=MESH,
        )

    def send(src, dst, device):
        copy = remote(src, dst, device)
        copy.start()
        return copy

    def on_plane(k):
        tz, ty = lax.rem(z + k // 4, 4), lax.rem(y + k % 4, 4)
        return {"z": tz, "y": ty}, tz * 4 + ty

    def on_line(k):
        return {
            "xl": 1 - xl if k & 1 else xl,
            "c": 1 - c if k & 2 else c,
            "xh": 1 - xh if k & 4 else xh,
        }

    core = {"c": 1 - c}
    pair = {"xl": 1 - xl}
    cut = {"xl": 1 - xl, "xh": 1 - xh}
    far_mate = {"xh": 1 - xh}

    gone = (1 - xl) * 2 + c
    load_b = []
    for k in range(4):
        q = lax.rem(gone + k, 4)
        rows_q = pl.ds(pl.multiple_of(q * quarter, quarter), quarter)
        load_b.append(pltpu.make_async_copy(bank_hbm.at[rows_q], bu.at[0, q], loc.at[1 + k]))
    load_w = pltpu.make_async_copy(hw_hbm, w.at[c], loc.at[0])
    load_b[0].start()
    load_w.start()
    for k in range(1, 4):
        load_b[k].start()

    barrier = pltpu.get_barrier_semaphore()
    for k in range(1, N_PLANE):
        pl.semaphore_signal(barrier, inc=1, device_id=on_plane(k)[0], device_id_type=MESH)
    for k in range(1, 8):
        pl.semaphore_signal(barrier, inc=1, device_id=on_line(k), device_id_type=MESH)

    def modulate(i, _):
        r = pl.ds(pl.multiple_of(i * 16, 16), 16)
        f = lat[r, :].astype(F32)
        inverse = lax.rsqrt(jnp.mean(f * f, axis=1, keepdims=True) + 1e-06)
        h = (f * inverse * (1.0 + scale[r, :].astype(F32)) + shift[r, :].astype(F32)).astype(BF16)
        hid[0, r, :] = h[:, :half]
        hid[1, r, :] = h[:, half:]
        return 0

    lax.fori_loop(0, rows // 16, modulate, 0)
    for p in range(N_PLANE // 2):
        for g in range(4):
            o = (g % 2) * strip + p * 128
            for j in range(tiles):
                hs[p, j, :, g * 128 : (g + 1) * 128] = hid[
                    g // 2, j * trows : (j + 1) * trows, o : o + 128
                ]
    for j in range(tiles):
        cols[j, me] = hs[me // 2, j]
    lhs[:rows] = hid[xl]

    def unit_rows(q):
        def step(i, _):
            r = pl.ds(pl.multiple_of(i * 64, 64), 64)
            b = bu[0, q, r, :].astype(F32)
            bu[0, q, r, :] = (b * lax.rsqrt(jnp.sum(b * b, axis=1, keepdims=True) + 1e-06)).astype(BF16)
            return 0

        lax.fori_loop(0, quarter // 64, step, 0)

    load_b[0].wait()
    own_q = xl * 2 + c
    pair_q = (1 - xl) * 2 + c
    per = quarter // CHUNKS
    unit_rows(gone)
    pl.semaphore_wait(barrier, N_PLANE - 1 + 7)

    upper, lower = pl.ds(0, hrows), pl.ds(hrows, hrows)
    send_h = [
        send(hid.at[1 - xl, upper], lhs.at[pl.ds(rows, hrows)], pair),
        send(hid.at[1 - xl, lower], lhs.at[pl.ds(rows + hrows, hrows)], cut),
    ]
    load_w.wait()
    send_w = send(w.at[c], w.at[c], core)

    def piece(i):
        return pl.ds(i * per, per)

    send_b = [remote(bu.at[0, gone, piece(i)], bu.at[1, gone, piece(i)], cut) for i in range(CHUNKS)]
    pass_core = [remote(bu.at[1, own_q, piece(i)], bu.at[1, own_q, piece(i)], core) for i in range(CHUNKS)]
    pass_pair = [remote(bu.at[1, own_q, piece(i)], bu.at[1, own_q, piece(i)], pair) for i in range(CHUNKS)]
    pass_last = [remote(bu.at[1, pair_q, piece(i)], bu.at[1, pair_q, piece(i)], core) for i in range(CHUNKS)]
    send_b[0].start()
    send_c = []
    for k in NEAREST:
        device, m = on_plane(k)
        send_c.append(send(hs.at[m // 2], cols.at[:, me], device))
    for k in range(1, 4):
        load_b[k].wait()
        unit_rows(lax.rem(gone + k, 4))

    send_w.wait()
    for copy in send_h:
        copy.wait()
    emb = jnp.dot(lhs[...], w[...].reshape(half, width), preferred_element_type=F32)
    ret[...] = emb[rows:]
    ue[...] = emb[:rows]
    send_e = [
        send(ret.at[upper], er.at[upper], pair),
        send(ret.at[lower], er.at[lower], cut),
    ]
    for i in range(1, CHUNKS):
        send_b[i].start()
    for copy in send_e:
        copy.wait()
    embed = ue[...] + er[...]
    length = jnp.sqrt(jnp.sum(embed * embed, axis=1, keepdims=True) + 1e-06)
    lens[...] = length
    unit = embed / length
    ue[...] = unit
    unit_b = unit.astype(BF16)
    pairt[:rows] = unit_b
    for j in range(tiles):
        units[j, me] = unit_b[j * trows : (j + 1) * trows]

    def along(h, second, d):
        if (h == 0) != second:
            return {"z": lax.rem(z + d, 4)}
        return {"y": lax.rem(y + d, 4)}

    def source(h, d):
        if h == 0:
            return lax.rem(z + 4 - d, 4) * 4 + y
        return z * 4 + lax.rem(y + 4 - d, 4)

    steps = (1, 3, 2)

    def gather(block):
        first, second = {}, []
        for d in steps:
            for h in range(2):
                first[h, d] = send(block(h, me), block(h, me), along(h, False, d))
        for d in steps:
            for h in range(2):
                second.append(send(block(h, me), block(h, me), along(h, True, d)))

        def forward():
            for d in steps:
                for h in range(2):
                    first[h, d].wait()
                    m = source(h, d)
                    for e in steps:
                        second.append(send(block(h, m), block(h, m), along(h, True, e)))

        def done():
            for copy in second:
                copy.wait()

        return forward, done

    def gather_relay(block, size):
        first, second, last = {}, {}, []
        for d in steps:
            for h in range(2):
                first[h, d] = send(block(h, me, 0, size), block(h, me, 0, size), along(h, False, d))
        for e in (1, 3):
            for h in range(2):
                second[h, 0, e] = send(block(h, me, 0, size), block(h, me, 0, size), along(h, True, e))

        def forward():
            for d in steps:
                for h in range(2):
                    first[h, d].wait()
                    m = source(h, d)
                    for e in (1, 3):
                        second[h, d, e] = send(
                            block(h, m, 0, size), block(h, m, 0, size), along(h, True, e)
                        )

        def relay():
            for d in (0,) + steps:
                for e in (1, 3):
                    for h in range(2):
                        second[h, d, e].wait()
                        dz, dy = (d, e) if h == 0 else (e, d)
                        m = lax.rem(z + 4 - dz, 4) * 4 + lax.rem(y + 4 - dy, 4)
                        o = 0 if e == 1 else size // 2
                        half_block = block(h, m, o, size // 2)
                        last.append(send(half_block, half_block, along(h, True, e)))

        def done():
            for copy in last:
                copy.wait()

        return forward, relay, done

    def gather_units(j):
        return gather(lambda h, m: units.at[j, m, :, pl.ds(h * (width // 2), width // 2)])

    flows = [gather_units(0), gather_units(1)]

    def pass_on(i):
        send_b[i].wait()
        pass_core[i].start()
        pass_pair[i].start()

    def pass_again(i):
        pass_pair[i].wait()
        pass_last[i].start()

    def weigh(slot, j, order, first):
        u = units[j].reshape(tile, width)
        total = None if first else acc[j].reshape(tile, width)
        for q in order:
            b = bu[slot, q]
            scores = lax.dot_general(u, b, (((1,), (1,)), ((), ())), preferred_element_type=F32)
            weight = jnp.exp(KERNEL_SCALE * scores).astype(BF16)
            term = jnp.dot(weight, b, preferred_element_type=F32)
            total = term if total is None else total + term
        acc[j] = total.reshape(4, 4, trows, width)

    batch = 2 * tiles * tile

    def finish(j):
        u = units[j].reshape(tile, width)
        t = pairt[...]
        scores = lax.dot_general(u, t, (((1,), (1,)), ((), ())), preferred_element_type=F32)
        row = lax.broadcasted_iota(jnp.int32, scores.shape, 0) - me * trows
        column = lax.broadcasted_iota(jnp.int32, scores.shape, 1) - j * trows
        same = jnp.logical_and(row == column, jnp.logical_and(column >= 0, column < trows))
        weight = jnp.where(same, F32(0.0), jnp.exp(KERNEL_SCALE * scores)).astype(BF16)
        total = jnp.dot(weight, t, preferred_element_type=F32)
        proof = total * (1.0 / (batch - 1)) - acc[j].reshape(tile, width) * (1.0 / (brows * 32))
        proof = proof.reshape(4, 4, trows, width)
        acc[j] = proof
        wide[j] = proof.astype(BF16)
        sends = {}
        for d in steps:
            tz, ty = lax.rem(z + d, 4), lax.rem(y + d, 4)
            sends[0, d] = send(wide.at[j, tz, :, :, left], landed.at[j, 0, d - 1], {"z": tz})
            sends[1, d] = send(wide.at[j, :, ty, :, right], landed.at[j, 1, d - 1], {"y": ty})
        return sends

    left, right = pl.ds(0, width // 2), pl.ds(width // 2, width // 2)

    def middle(j, firsts):
        sends = []
        for h in range(2):
            part_sum = acc[j, z, :, :, left] if h == 0 else acc[j, :, y, :, right]
            for d in steps:
                firsts[h, d].wait()
                part_sum = part_sum + landed[j, h, d - 1].astype(F32)
            keep[...] = part_sum
            mids[j, h] = part_sum.astype(BF16)
            acc[j, 0, h, :, left] = keep[y if h == 0 else z]
            for e in steps:
                to = lax.rem((y if h == 0 else z) + e, 4)
                sends.append(
                    send(mids.at[j, h, to], landed2.at[j, h, e - 1], {"y": to} if h == 0 else {"z": to})
                )
        return sends

    def land(j, sends):
        for copy in sends:
            copy.wait()
        halves = []
        for h in range(2):
            own_sum = acc[j, 0, h, :, left]
            for e in steps:
                own_sum = own_sum + landed2[j, h, e - 1].astype(F32)
            halves.append(own_sum)
        proof = jnp.concatenate(halves, axis=1)
        r = slice(j * trows, (j + 1) * trows)
        unit = ue[r, :]
        radial = jnp.sum(unit * proof, axis=1, keepdims=True)
        grads[j, me] = ((proof - unit * radial) / lens[r, :]).astype(BF16)
        return gather_relay(
            lambda h, m, o, n: grads.at[j, m, :, pl.ds(h * (width // 2) + o, n)], width // 2
        )

    own = (0, 1, 2, 3)
    core_q = xl * 2 + 1 - c
    late_q = (pair_q, (1 - xl) * 2 + 1 - c)
    pass_on(0)
    flows[0][0]()
    flows.append(gather_units(2))
    pass_on(1)
    flows[1][0]()
    flows.append(gather_units(3))
    pass_on(2)
    flows[0][1]()
    pass_on(3)
    weigh(0, 0, own, True)
    flows[2][0]()
    pass_on(4)
    pass_again(0)
    pass_again(1)
    flows[1][1]()
    weigh(0, 1, own, True)
    flows[3][0]()
    pass_on(5)
    pass_again(2)
    flows[2][1]()
    weigh(0, 2, own, True)
    pass_on(6)
    pass_again(3)
    flows[3][1]()
    weigh(0, 3, own, True)
    pass_on(7)
    send_m = send(pairt.at[pl.ds(0, rows)], pairt.at[pl.ds(rows, rows)], far_mate)
    pass_again(4)
    weigh(1, 2, (own_q,), False)
    weigh(1, 3, (own_q,), False)
    pass_again(5)
    weigh(1, 0, (own_q,), False)
    weigh(1, 1, (own_q,), False)
    pass_again(6)
    for i in range(CHUNKS):
        pass_core[i].wait()
    weigh(1, 0, (core_q,), False)
    weigh(1, 1, (core_q,), False)
    pass_again(7)
    weigh(1, 2, (core_q,), False)
    weigh(1, 3, (core_q,), False)
    for i in range(CHUNKS):
        pass_last[i].wait()
    send_m.wait()
    weigh(1, 0, late_q, False)
    send_p = [finish(0)]
    weigh(1, 1, late_q, False)
    send_p.append(finish(1))
    weigh(1, 2, late_q, False)
    send_p.append(finish(2))
    middles = [middle(0, send_p[0])]
    weigh(1, 3, late_q, False)
    send_p.append(finish(3))
    middles.append(middle(1, send_p[1]))
    spread = [land(0, middles[0])]
    middles.append(middle(2, send_p[2]))
    spread.append(land(1, middles[1]))
    middles.append(middle(3, send_p[3]))
    spread[0][0]()
    spread.append(land(2, middles[2]))
    spread[1][0]()
    spread[0][1]()
    spread.append(land(3, middles[3]))
    spread[2][0]()
    spread[1][1]()
    spread[3][0]()
    spread[2][1]()
    spread[3][1]()
    for copy in send_c:
        copy.wait()
    for j in range(tiles):
        spread[j][2]()

    feats = cols[...].reshape(N_PLANE * rows, 512).T
    lane = lax.rem(y, 2) * 64

    def strip_of(axl, ac):
        return pl.ds(pl.multiple_of((axl * 2 + ac) * 128 + lane, 64), 64)

    swap = []
    for side in (left, right):
        samples_grads = grads[:, :, :, side].reshape(N_PLANE * rows, width // 2)
        part[:, side] = jnp.dot(feats, samples_grads, preferred_element_type=F32)
        swap.append([send(part.at[strip_of(a, 1 - c), side], mine.at[a, :, side], core) for a in range(2)])
    here = pl.ds(pl.multiple_of(xh * 32, 32), 32)
    send_x = []
    for h, side in enumerate((left, right)):
        for a in range(2):
            swap[h][a].wait()
            total = mine[a, :, side] + part[strip_of(a, c), side]
            mine[a, :, side] = total
            xout[h, a] = total.astype(BF16)
        for k in (1, 5, 4):
            to = on_line(k)
            block = xout.at[h, to["xl"], pl.ds(pl.multiple_of(to["xh"] * 32, 32), 32)]
            send_x.append(send(block, xin.at[len(send_x)], to))
    fold = jnp.zeros((8, 128), F32)
    for h, side in enumerate((left, right)):
        total = mine[xl, here, side]
        for i in range(3):
            send_x[h * 3 + i].wait()
            total = total + xin[h * 3 + i].astype(F32)
        grad[:, side] = total
        squares = total * total
        for a in range(4):
            for b in range(width // 256):
                fold = fold + squares[a * 8 : a * 8 + 8, b * 128 : b * 128 + 128]
    q1[...] = fold
    send_q = []
    for k in range(1, 8):
        send_q.append(send(q1, q1in.at[k - 1], on_line(k)))
    for k in range(1, 8):
        send_q[k - 1].wait()
        fold = fold + q1in[k - 1]
    q2[...] = fold
    send_q = []
    for k in range(1, N_PLANE):
        send_q.append(send(q2, q2in.at[k - 1], on_plane(k)[0]))
    for k in range(1, N_PLANE):
        send_q[k - 1].wait()
        fold = fold + q2in[k - 1]
    mean = jnp.sum(jnp.sum(fold, axis=1, keepdims=True), axis=0, keepdims=True) / (
        4 * strip * width
    )
    factor[...] = jnp.broadcast_to(lax.rsqrt(mean + 1e-06), factor.shape)


def local(latents, shift, scale_mod, head_weight, bank):
    rows, depth = latents.shape
    width = head_weight.shape[1]
    brows = bank.shape[0]
    vmem = pl.BlockSpec(memory_space=pltpu.VMEM)
    hbm = pl.BlockSpec(memory_space=pl.ANY)
    n_sems = 5 + 4 * CHUNKS + 15 + 4 * 30 + 1 + 4 * 12 + 4 * 38 + 10 + 7 + 15
    gradient, factor = pl.pallas_call(
        kernel,
        out_shape=(
            jax.ShapeDtypeStruct((depth // 128, width), F32),
            jax.ShapeDtypeStruct((1, 128), F32),
        ),
        in_specs=[vmem, vmem, vmem, hbm, hbm],
        out_specs=(vmem, vmem),
        scratch_shapes=[
            pltpu.VMEM((2, rows, depth // 2), BF16),
            pltpu.VMEM((2 * rows, depth // 2), BF16),
            pltpu.VMEM((2, depth // 4, width), BF16),
            pltpu.VMEM((rows, width), F32),
            pltpu.VMEM((rows, width), F32),
            pltpu.VMEM((rows, width), F32),
            pltpu.VMEM((rows, 1), F32),
            pltpu.VMEM((4, N_PLANE, rows // 4, width), BF16),
            pltpu.VMEM((2 * rows, width), BF16),
            pltpu.VMEM((2, 4, brows // 4, width), BF16),
            pltpu.VMEM((4, 4, 4, rows // 4, width), F32),
            pltpu.VMEM((4, 4, 4, rows // 4, width), BF16),
            pltpu.VMEM((4, 2, 3, 4, rows // 4, width // 2), BF16),
            pltpu.VMEM((4, 2, 4, rows // 4, width // 2), BF16),
            pltpu.VMEM((4, 2, 3, rows // 4, width // 2), BF16),
            pltpu.VMEM((4, rows // 4, width // 2), F32),
            pltpu.VMEM((N_PLANE // 2, 4, rows // 4, 512), BF16),
            pltpu.VMEM((4, N_PLANE, rows // 4, 512), BF16),
            pltpu.VMEM((4, N_PLANE, rows // 4, width), BF16),
            pltpu.VMEM((512, width), F32),
            pltpu.VMEM((2, 64, width), F32),
            pltpu.VMEM((6, 32, width // 2), BF16),
            pltpu.VMEM((2, 2, 64, width // 2), BF16),
            pltpu.VMEM((8, 128), F32),
            pltpu.VMEM((7, 8, 128), F32),
            pltpu.VMEM((8, 128), F32),
            pltpu.VMEM((15, 8, 128), F32),
            pltpu.SemaphoreType.DMA((5,)),
            pltpu.SemaphoreType.DMA((n_sems,)),
            pltpu.SemaphoreType.DMA((n_sems,)),
        ],
        compiler_params=pltpu.CompilerParams(
            collective_id=0, has_side_effects=True, vmem_limit_bytes=60 * 1024 * 1024
        ),
        name="mmd_step",
    )(latents, shift, scale_mod, head_weight, bank)
    return gradient * factor[0, 0]


def solution(mesh):
    torus = Mesh(mesh.devices.reshape(2, 2, 4, 4, 2), AXES)
    return jax.shard_map(
        local,
        mesh=torus,
        in_specs=(P(AXES, None), P(AXES, None), P(AXES, None), P(("xl", "c"), None), P(("z", "y", "xh"), None)),
        out_specs=P(AXES, None),
        check_vma=False,
    )
```

```python
import functools

import jax
import jax.numpy as jnp
from jax import lax
from jax.experimental import pallas as pl
from jax.experimental.pallas import tpu as pltpu
from jax.sharding import Mesh
from jax.sharding import PartitionSpec as P

AXES = ("xl", "c", "z", "y", "xh")
MESH = pl.DeviceIdType.MESH
F32 = jnp.float32
BF16 = jnp.bfloat16
KERNEL_SCALE = 32.0
N_PLANE = 16
CHUNKS = 8
NEAREST = sorted(range(1, 16), key=lambda k: min(k // 4, 4 - k // 4) + min(k % 4, 4 - k % 4))


def kernel(
    lat_hbm, shift_hbm, scale_hbm, hw_hbm, bank_hbm, grad, factor,
    lat, shift, scale, hid, lhs, w, ret, er, ue, lens, units, pairt, bu, acc, wide, landed, mids, landed2, keep, hs, cols, grads, part, mine,
    xin, xout, q1, q1in, q2, q2in, loc, ss, rs,
):
    xl, c, z, y, xh = (lax.axis_index(a) for a in AXES)
    me = z * 4 + y
    rows, width = ret.shape
    half = hid.shape[2]
    strip = half // 2
    brows = bu.shape[1] * bu.shape[2]
    quarter = bu.shape[2]
    tiles, _, trows = units.shape[:3]
    tile = N_PLANE * trows
    hrows = rows // 2

    ids = iter(range(ss.shape[0]))

    def remote(src, dst, device):
        i = next(ids)
        return pltpu.make_async_remote_copy(
            src_ref=src, dst_ref=dst, send_sem=ss.at[i], recv_sem=rs.at[i],
            device_id=device, device_id_type=MESH,
        )

    def send(src, dst, device):
        copy = remote(src, dst, device)
        copy.start()
        return copy

    def on_plane(k):
        tz, ty = lax.rem(z + k // 4, 4), lax.rem(y + k % 4, 4)
        return {"z": tz, "y": ty}, tz * 4 + ty

    def on_line(k):
        return {
            "xl": 1 - xl if k & 1 else xl,
            "c": 1 - c if k & 2 else c,
            "xh": 1 - xh if k & 4 else xh,
        }

    core = {"c": 1 - c}
    pair = {"xl": 1 - xl}
    cut = {"xl": 1 - xl, "xh": 1 - xh}
    far_mate = {"xh": 1 - xh}

    load_f = [
        pltpu.make_async_copy(src, dst, loc.at[5 + n])
        for n, (src, dst) in enumerate(((lat_hbm, lat), (shift_hbm, shift), (scale_hbm, scale)))
    ]
    for copy in load_f:
        copy.start()
    barrier = pltpu.get_barrier_semaphore()
    for k in range(1, N_PLANE):
        pl.semaphore_signal(barrier, inc=1, device_id=on_plane(k)[0], device_id_type=MESH)
    for k in range(1, 8):
        pl.semaphore_signal(barrier, inc=1, device_id=on_line(k), device_id_type=MESH)

    gone = (1 - xl) * 2 + c
    load_b = []
    for k in range(4):
        q = lax.rem(gone + k, 4)
        rows_q = pl.ds(pl.multiple_of(q * quarter, quarter), quarter)
        load_b.append(pltpu.make_async_copy(bank_hbm.at[rows_q], bu.at[0, q], loc.at[1 + k]))
    load_w = pltpu.make_async_copy(hw_hbm, w.at[c], loc.at[0])
    load_b[0].start()
    load_w.start()
    for k in range(1, 4):
        load_b[k].start()

    def modulate(i, _):
        r = pl.ds(pl.multiple_of(i * 16, 16), 16)
        f = lat[r, :].astype(F32)
        inverse = lax.rsqrt(jnp.mean(f * f, axis=1, keepdims=True) + 1e-06)
        h = (f * inverse * (1.0 + scale[r, :].astype(F32)) + shift[r, :].astype(F32)).astype(BF16)
        hid[0, r, :] = h[:, :half]
        hid[1, r, :] = h[:, half:]
        return 0

    for copy in load_f:
        copy.wait()
    lax.fori_loop(0, rows // 16, modulate, 0)
    for p in range(N_PLANE // 2):
        for g in range(4):
            o = (g % 2) * strip + p * 128
            for j in range(tiles):
                hs[p, j, :, g * 128 : (g + 1) * 128] = hid[
                    g // 2, j * trows : (j + 1) * trows, o : o + 128
                ]
    for j in range(tiles):
        cols[j, me] = hs[me // 2, j]
    lhs[:rows] = hid[xl]

    def unit_rows(q):
        def step(i, _):
            r = pl.ds(pl.multiple_of(i * 64, 64), 64)
            b = bu[0, q, r, :].astype(F32)
            bu[0, q, r, :] = (b * lax.rsqrt(jnp.sum(b * b, axis=1, keepdims=True) + 1e-06)).astype(BF16)
            return 0

        lax.fori_loop(0, quarter // 64, step, 0)

    load_b[0].wait()
    own_q = xl * 2 + c
    pair_q = (1 - xl) * 2 + c
    per = quarter // CHUNKS
    unit_rows(gone)
    pl.semaphore_wait(barrier, N_PLANE - 1 + 7)

    upper, lower = pl.ds(0, hrows), pl.ds(hrows, hrows)
    send_h = [
        send(hid.at[1 - xl, upper], lhs.at[pl.ds(rows, hrows)], pair),
        send(hid.at[1 - xl, lower], lhs.at[pl.ds(rows + hrows, hrows)], cut),
    ]
    load_w.wait()
    send_w = send(w.at[c], w.at[c], core)

    def piece(i):
        return pl.ds(i * per, per)

    send_b = [remote(bu.at[0, gone, piece(i)], bu.at[1, gone, piece(i)], cut) for i in range(CHUNKS)]
    pass_core = [remote(bu.at[1, own_q, piece(i)], bu.at[1, own_q, piece(i)], core) for i in range(CHUNKS)]
    pass_pair = [remote(bu.at[1, own_q, piece(i)], bu.at[1, own_q, piece(i)], pair) for i in range(CHUNKS)]
    pass_last = [remote(bu.at[1, pair_q, piece(i)], bu.at[1, pair_q, piece(i)], core) for i in range(CHUNKS)]
    send_b[0].start()
    send_c = []
    for k in NEAREST:
        device, m = on_plane(k)
        send_c.append(send(hs.at[m // 2], cols.at[:, me], device))
    for k in range(1, 4):
        load_b[k].wait()
        unit_rows(lax.rem(gone + k, 4))

    send_w.wait()
    for copy in send_h:
        copy.wait()
    emb = jnp.dot(lhs[...], w[...].reshape(half, width), preferred_element_type=F32)
    ret[...] = emb[rows:]
    ue[...] = emb[:rows]
    send_e = [
        send(ret.at[upper], er.at[upper], pair),
        send(ret.at[lower], er.at[lower], cut),
    ]
    for i in range(1, CHUNKS):
        send_b[i].start()
    for copy in send_e:
        copy.wait()
    embed = ue[...] + er[...]
    length = jnp.sqrt(jnp.sum(embed * embed, axis=1, keepdims=True) + 1e-06)
    lens[...] = length
    unit = embed / length
    ue[...] = unit
    unit_b = unit.astype(BF16)
    pairt[:rows] = unit_b
    for j in range(tiles):
        units[j, me] = unit_b[j * trows : (j + 1) * trows]

    def along(h, second, d):
        if (h == 0) != second:
            return {"z": lax.rem(z + d, 4)}
        return {"y": lax.rem(y + d, 4)}

    def source(h, d):
        if h == 0:
            return lax.rem(z + 4 - d, 4) * 4 + y
        return z * 4 + lax.rem(y + 4 - d, 4)

    steps = (1, 3, 2)

    def gather(block):
        first, second = {}, []
        for d in steps:
            for h in range(2):
                first[h, d] = send(block(h, me), block(h, me), along(h, False, d))
        for d in steps:
            for h in range(2):
                second.append(send(block(h, me), block(h, me), along(h, True, d)))

        def forward():
            for d in steps:
                for h in range(2):
                    first[h, d].wait()
                    m = source(h, d)
                    for e in steps:
                        second.append(send(block(h, m), block(h, m), along(h, True, e)))

        def done():
            for copy in second:
                copy.wait()

        return forward, done

    def gather_relay(block, size):
        first, second, last = {}, {}, []
        for d in steps:
            for h in range(2):
                first[h, d] = send(block(h, me, 0, size), block(h, me, 0, size), along(h, False, d))
        for e in (1, 3):
            for h in range(2):
                second[h, 0, e] = send(block(h, me, 0, size), block(h, me, 0, size), along(h, True, e))

        def forward():
            for d in steps:
                for h in range(2):
                    first[h, d].wait()
                    m = source(h, d)
                    for e in (1, 3):
                        second[h, d, e] = send(
                            block(h, m, 0, size), block(h, m, 0, size), along(h, True, e)
                        )

        def relay():
            for d in (0,) + steps:
                for e in (1, 3):
                    for h in range(2):
                        second[h, d, e].wait()
                        dz, dy = (d, e) if h == 0 else (e, d)
                        m = lax.rem(z + 4 - dz, 4) * 4 + lax.rem(y + 4 - dy, 4)
                        o = 0 if e == 1 else size // 2
                        half_block = block(h, m, o, size // 2)
                        last.append(send(half_block, half_block, along(h, True, e)))

        def done():
            for copy in last:
                copy.wait()

        return forward, relay, done

    def gather_units(j):
        return gather(lambda h, m: units.at[j, m, :, pl.ds(h * (width // 2), width // 2)])

    flows = [gather_units(0), gather_units(1)]

    def pass_on(i):
        send_b[i].wait()
        pass_core[i].start()
        pass_pair[i].start()

    def pass_again(i):
        pass_pair[i].wait()
        pass_last[i].start()

    def weigh(slot, j, order, first):
        u = units[j].reshape(tile, width)
        total = None if first else acc[j].reshape(tile, width)
        for q in order:
            b = bu[slot, q]
            scores = lax.dot_general(u, b, (((1,), (1,)), ((), ())), preferred_element_type=F32)
            weight = jnp.exp(KERNEL_SCALE * scores).astype(BF16)
            term = jnp.dot(weight, b, preferred_element_type=F32)
            total = term if total is None else total + term
        acc[j] = total.reshape(4, 4, trows, width)

    batch = 2 * tiles * tile

    def finish(j):
        u = units[j].reshape(tile, width)
        t = pairt[...]
        scores = lax.dot_general(u, t, (((1,), (1,)), ((), ())), preferred_element_type=F32)
        row = lax.broadcasted_iota(jnp.int32, scores.shape, 0) - me * trows
        column = lax.broadcasted_iota(jnp.int32, scores.shape, 1) - j * trows
        same = jnp.logical_and(row == column, jnp.logical_and(column >= 0, column < trows))
        weight = jnp.where(same, F32(0.0), jnp.exp(KERNEL_SCALE * scores)).astype(BF16)
        total = jnp.dot(weight, t, preferred_element_type=F32)
        proof = total * (1.0 / (batch - 1)) - acc[j].reshape(tile, width) * (1.0 / (brows * 32))
        proof = proof.reshape(4, 4, trows, width)
        acc[j] = proof
        wide[j] = proof.astype(BF16)
        sends = {}
        for d in steps:
            tz, ty = lax.rem(z + d, 4), lax.rem(y + d, 4)
            sends[0, d] = send(wide.at[j, tz, :, :, left], landed.at[j, 0, d - 1], {"z": tz})
            sends[1, d] = send(wide.at[j, :, ty, :, right], landed.at[j, 1, d - 1], {"y": ty})
        return sends

    left, right = pl.ds(0, width // 2), pl.ds(width // 2, width // 2)

    def middle(j, firsts):
        sends = []
        for h in range(2):
            part_sum = acc[j, z, :, :, left] if h == 0 else acc[j, :, y, :, right]
            for d in steps:
                firsts[h, d].wait()
                part_sum = part_sum + landed[j, h, d - 1].astype(F32)
            keep[...] = part_sum
            mids[j, h] = part_sum.astype(BF16)
            acc[j, 0, h, :, left] = keep[y if h == 0 else z]
            for e in steps:
                to = lax.rem((y if h == 0 else z) + e, 4)
                sends.append(
                    send(mids.at[j, h, to], landed2.at[j, h, e - 1], {"y": to} if h == 0 else {"z": to})
                )
        return sends

    def land(j, sends):
        for copy in sends:
            copy.wait()
        halves = []
        for h in range(2):
            own_sum = acc[j, 0, h, :, left]
            for e in steps:
                own_sum = own_sum + landed2[j, h, e - 1].astype(F32)
            halves.append(own_sum)
        proof = jnp.concatenate(halves, axis=1)
        r = slice(j * trows, (j + 1) * trows)
        unit = ue[r, :]
        radial = jnp.sum(unit * proof, axis=1, keepdims=True)
        grads[j, me] = ((proof - unit * radial) / lens[r, :]).astype(BF16)
        if j == tiles - 1:
            return gather(lambda h, m: grads.at[j, m, :, pl.ds(h * (width // 2), width // 2)])
        return gather_relay(
            lambda h, m, o, n: grads.at[j, m, :, pl.ds(h * (width // 2) + o, n)], width // 2
        )

    own = (0, 1, 2, 3)
    core_q = xl * 2 + 1 - c
    late_q = (pair_q, (1 - xl) * 2 + 1 - c)
    pass_on(0)
    flows[0][0]()
    flows.append(gather_units(2))
    pass_on(1)
    flows[1][0]()
    flows.append(gather_units(3))
    pass_on(2)
    flows[0][1]()
    pass_on(3)
    weigh(0, 0, own, True)
    flows[2][0]()
    pass_on(4)
    pass_again(0)
    pass_again(1)
    flows[1][1]()
    weigh(0, 1, own, True)
    flows[3][0]()
    pass_again(2)
    flows[2][1]()
    weigh(0, 2, (0, 1), True)
    pass_on(5)
    weigh(0, 2, (2, 3), False)
    pass_on(6)
    pass_again(3)
    flows[3][1]()
    weigh(0, 3, (0, 1), True)
    pass_on(7)
    weigh(0, 3, (2, 3), False)
    send_m = send(pairt.at[pl.ds(0, rows)], pairt.at[pl.ds(rows, rows)], far_mate)
    pass_again(4)
    weigh(1, 2, (own_q,), False)
    weigh(1, 3, (own_q,), False)
    pass_again(5)
    weigh(1, 0, (own_q,), False)
    weigh(1, 1, (own_q,), False)
    for i in range(CHUNKS):
        pass_core[i].wait()
    pass_again(6)
    weigh(1, 0, (core_q,), False)
    weigh(1, 1, (core_q,), False)
    pass_again(7)
    weigh(1, 2, (core_q,), False)
    weigh(1, 3, (core_q,), False)
    for i in range(CHUNKS):
        pass_last[i].wait()
    send_m.wait()
    weigh(1, 0, late_q, False)
    send_p = [finish(0)]
    weigh(1, 1, late_q, False)
    send_p.append(finish(1))
    weigh(1, 2, late_q, False)
    send_p.append(finish(2))
    middles = [middle(0, send_p[0])]
    weigh(1, 3, late_q, False)
    send_p.append(finish(3))
    middles.append(middle(1, send_p[1]))
    spread = [land(0, middles[0])]
    middles.append(middle(2, send_p[2]))
    spread.append(land(1, middles[1]))
    middles.append(middle(3, send_p[3]))
    spread[0][0]()
    spread.append(land(2, middles[2]))
    spread[1][0]()
    spread[0][1]()
    spread.append(land(3, middles[3]))
    spread[2][0]()
    spread[1][1]()
    spread[3][0]()
    spread[2][1]()
    for copy in send_c:
        copy.wait()
    for j in range(tiles):
        spread[j][-1]()

    feats = cols[...].reshape(N_PLANE * rows, 512).T
    lane = lax.rem(y, 2) * 64

    def strip_of(axl, ac):
        return pl.ds(pl.multiple_of((axl * 2 + ac) * 128 + lane, 64), 64)

    swap = []
    for side in (left, right):
        samples_grads = grads[:, :, :, side].reshape(N_PLANE * rows, width // 2)
        part[:, side] = jnp.dot(feats, samples_grads, preferred_element_type=F32)
        swap.append([send(part.at[strip_of(a, 1 - c), side], mine.at[a, :, side], core) for a in range(2)])
    here = pl.ds(pl.multiple_of(xh * 32, 32), 32)
    send_x = []
    for h, side in enumerate((left, right)):
        for a in range(2):
            swap[h][a].wait()
            total = mine[a, :, side] + part[strip_of(a, c), side]
            mine[a, :, side] = total
            xout[h, a] = total.astype(BF16)
        for k in (1, 5, 4):
            to = on_line(k)
            block = xout.at[h, to["xl"], pl.ds(pl.multiple_of(to["xh"] * 32, 32), 32)]
            send_x.append(send(block, xin.at[len(send_x)], to))
    fold = jnp.zeros((8, 128), F32)
    for h, side in enumerate((left, right)):
        total = mine[xl, here, side]
        for i in range(3):
            send_x[h * 3 + i].wait()
            total = total + xin[h * 3 + i].astype(F32)
        grad[:, side] = total
        squares = total * total
        for a in range(4):
            for b in range(width // 256):
                fold = fold + squares[a * 8 : a * 8 + 8, b * 128 : b * 128 + 128]
    q1[...] = fold
    send_q = []
    for k in range(1, 8):
        send_q.append(send(q1, q1in.at[k - 1], on_line(k)))
    for k in range(1, 8):
        send_q[k - 1].wait()
        fold = fold + q1in[k - 1]
    q2[...] = fold
    send_q = []
    for k in range(1, N_PLANE):
        send_q.append(send(q2, q2in.at[k - 1], on_plane(k)[0]))
    for k in range(1, N_PLANE):
        send_q[k - 1].wait()
        fold = fold + q2in[k - 1]
    mean = jnp.sum(jnp.sum(fold, axis=1, keepdims=True), axis=0, keepdims=True) / (
        4 * strip * width
    )
    factor[...] = jnp.broadcast_to(lax.rsqrt(mean + 1e-06), factor.shape)


def local(latents, shift, scale_mod, head_weight, bank):
    rows, depth = latents.shape
    width = head_weight.shape[1]
    brows = bank.shape[0]
    vmem = pl.BlockSpec(memory_space=pltpu.VMEM)
    hbm = pl.BlockSpec(memory_space=pl.ANY)
    n_sems = 5 + 4 * CHUNKS + 15 + 4 * 30 + 1 + 4 * 12 + 3 * 38 + 30 + 10 + 7 + 15
    gradient, factor = pl.pallas_call(
        kernel,
        out_shape=(
            jax.ShapeDtypeStruct((depth // 128, width), F32),
            jax.ShapeDtypeStruct((1, 128), F32),
        ),
        in_specs=[hbm] * 5,
        out_specs=(vmem, vmem),
        scratch_shapes=[
            pltpu.VMEM((rows, depth), BF16),
            pltpu.VMEM((rows, depth), BF16),
            pltpu.VMEM((rows, depth), BF16),
            pltpu.VMEM((2, rows, depth // 2), BF16),
            pltpu.VMEM((2 * rows, depth // 2), BF16),
            pltpu.VMEM((2, depth // 4, width), BF16),
            pltpu.VMEM((rows, width), F32),
            pltpu.VMEM((rows, width), F32),
            pltpu.VMEM((rows, width), F32),
            pltpu.VMEM((rows, 1), F32),
            pltpu.VMEM((4, N_PLANE, rows // 4, width), BF16),
            pltpu.VMEM((2 * rows, width), BF16),
            pltpu.VMEM((2, 4, brows // 4, width), BF16),
            pltpu.VMEM((4, 4, 4, rows // 4, width), F32),
            pltpu.VMEM((4, 4, 4, rows // 4, width), BF16),
            pltpu.VMEM((4, 2, 3, 4, rows // 4, width // 2), BF16),
            pltpu.VMEM((4, 2, 4, rows // 4, width // 2), BF16),
            pltpu.VMEM((4, 2, 3, rows // 4, width // 2), BF16),
            pltpu.VMEM((4, rows // 4, width // 2), F32),
            pltpu.VMEM((N_PLANE // 2, 4, rows // 4, 512), BF16),
            pltpu.VMEM((4, N_PLANE, rows // 4, 512), BF16),
            pltpu.VMEM((4, N_PLANE, rows // 4, width), BF16),
            pltpu.VMEM((512, width), F32),
            pltpu.VMEM((2, 64, width), F32),
            pltpu.VMEM((6, 32, width // 2), BF16),
            pltpu.VMEM((2, 2, 64, width // 2), BF16),
            pltpu.VMEM((8, 128), F32),
            pltpu.VMEM((7, 8, 128), F32),
            pltpu.VMEM((8, 128), F32),
            pltpu.VMEM((15, 8, 128), F32),
            pltpu.SemaphoreType.DMA((8,)),
            pltpu.SemaphoreType.DMA((n_sems,)),
            pltpu.SemaphoreType.DMA((n_sems,)),
        ],
        compiler_params=pltpu.CompilerParams(
            collective_id=0, has_side_effects=True, vmem_limit_bytes=60 * 1024 * 1024
        ),
        name="mmd_step",
    )(latents, shift, scale_mod, head_weight, bank)
    return gradient * factor[0, 0]


def solution(mesh):
    torus = Mesh(mesh.devices.reshape(2, 2, 4, 4, 2), AXES)
    return jax.shard_map(
        local,
        mesh=torus,
        in_specs=(P(AXES, None), P(AXES, None), P(AXES, None), P(("xl", "c"), None), P(("z", "y", "xh"), None)),
        out_specs=P(AXES, None),
        check_vma=False,
    )
```

```python
import functools

import jax
import jax.numpy as jnp
from jax import lax
from jax.experimental import pallas as pl
from jax.experimental.pallas import tpu as pltpu
from jax.sharding import Mesh
from jax.sharding import PartitionSpec as P

AXES = ("xl", "c", "z", "y", "xh")
MESH = pl.DeviceIdType.MESH
F32 = jnp.float32
BF16 = jnp.bfloat16
KERNEL_SCALE = 32.0
N_PLANE = 16
CHUNKS = 8
NEAREST = sorted(range(1, 16), key=lambda k: min(k // 4, 4 - k // 4) + min(k % 4, 4 - k % 4))


def kernel(
    lat_hbm, shift_hbm, scale_hbm, hw_hbm, bank_hbm, grad, factor,
    lat, shift, scale, hid, lhs, w, ret, er, ue, lens, units, pairt, bu, acc, wide, landed, mids, landed2, keep, hs, cols, grads, part, mine,
    xin, xout, q1, q1in, q2, q2in, loc, ss, rs,
):
    xl, c, z, y, xh = (lax.axis_index(a) for a in AXES)
    me = z * 4 + y
    rows, width = ret.shape
    half = hid.shape[2]
    strip = half // 2
    brows = bu.shape[1] * bu.shape[2]
    quarter = bu.shape[2]
    tiles, _, trows = units.shape[:3]
    tile = N_PLANE * trows
    hrows = rows // 2

    ids = iter(range(ss.shape[0]))

    def remote(src, dst, device):
        i = next(ids)
        return pltpu.make_async_remote_copy(
            src_ref=src, dst_ref=dst, send_sem=ss.at[i], recv_sem=rs.at[i],
            device_id=device, device_id_type=MESH,
        )

    def send(src, dst, device):
        copy = remote(src, dst, device)
        copy.start()
        return copy

    def on_plane(k):
        tz, ty = lax.rem(z + k // 4, 4), lax.rem(y + k % 4, 4)
        return {"z": tz, "y": ty}, tz * 4 + ty

    def on_line(k):
        return {
            "xl": 1 - xl if k & 1 else xl,
            "c": 1 - c if k & 2 else c,
            "xh": 1 - xh if k & 4 else xh,
        }

    core = {"c": 1 - c}
    pair = {"xl": 1 - xl}
    cut = {"xl": 1 - xl, "xh": 1 - xh}
    far_mate = {"xh": 1 - xh}

    parts = rows // 16
    load_f = []
    for i in range(parts):
        for n, (src, dst) in enumerate(((lat_hbm, lat), (shift_hbm, shift), (scale_hbm, scale))):
            r = pl.ds(i * 16, 16)
            load_f.append(pltpu.make_async_copy(src.at[r], dst.at[r], loc.at[5 + i * 3 + n]))
            load_f[-1].start()
    barrier = pltpu.get_barrier_semaphore()
    for k in range(1, N_PLANE):
        pl.semaphore_signal(barrier, inc=1, device_id=on_plane(k)[0], device_id_type=MESH)
    for k in range(1, 8):
        pl.semaphore_signal(barrier, inc=1, device_id=on_line(k), device_id_type=MESH)

    gone = (1 - xl) * 2 + c
    load_b = []
    for k in range(4):
        q = lax.rem(gone + k, 4)
        rows_q = pl.ds(pl.multiple_of(q * quarter, quarter), quarter)
        load_b.append(pltpu.make_async_copy(bank_hbm.at[rows_q], bu.at[0, q], loc.at[1 + k]))
    load_w = pltpu.make_async_copy(hw_hbm, w.at[c], loc.at[0])
    load_b[0].start()
    load_w.start()
    for k in range(1, 4):
        load_b[k].start()

    for i in range(parts):
        for n in range(3):
            load_f[i * 3 + n].wait()
        r = slice(i * 16, i * 16 + 16)
        f = lat[r, :].astype(F32)
        inverse = lax.rsqrt(jnp.mean(f * f, axis=1, keepdims=True) + 1e-06)
        h = (f * inverse * (1.0 + scale[r, :].astype(F32)) + shift[r, :].astype(F32)).astype(BF16)
        hid[0, r, :] = h[:, :half]
        hid[1, r, :] = h[:, half:]
    pl.semaphore_wait(barrier, N_PLANE - 1 + 7)

    upper, lower = pl.ds(0, hrows), pl.ds(hrows, hrows)
    send_h = [
        send(hid.at[1 - xl, upper], lhs.at[pl.ds(rows, hrows)], pair),
        send(hid.at[1 - xl, lower], lhs.at[pl.ds(rows + hrows, hrows)], cut),
    ]
    def unit_rows(q, lo, hi):
        def step(i, _):
            r = pl.ds(pl.multiple_of(i * 64, 64), 64)
            b = bu[0, q, r, :].astype(F32)
            bu[0, q, r, :] = (b * lax.rsqrt(jnp.sum(b * b, axis=1, keepdims=True) + 1e-06)).astype(BF16)
            return 0

        lax.fori_loop(lo, hi, step, 0)

    load_b[0].wait()
    own_q = xl * 2 + c
    pair_q = (1 - xl) * 2 + c
    per = quarter // CHUNKS
    unit_rows(gone, 0, 1)

    def piece(i):
        return pl.ds(i * per, per)

    send_b = [remote(bu.at[0, gone, piece(i)], bu.at[1, gone, piece(i)], cut) for i in range(CHUNKS)]
    pass_core = [remote(bu.at[1, own_q, piece(i)], bu.at[1, own_q, piece(i)], core) for i in range(CHUNKS)]
    pass_pair = [remote(bu.at[1, own_q, piece(i)], bu.at[1, own_q, piece(i)], pair) for i in range(CHUNKS)]
    pass_last = [remote(bu.at[1, pair_q, piece(i)], bu.at[1, pair_q, piece(i)], core) for i in range(CHUNKS)]
    send_b[0].start()
    load_w.wait()
    send_w = send(w.at[c], w.at[c], core)
    for p in range(N_PLANE // 2):
        for g in range(4):
            o = (g % 2) * strip + p * 128
            for j in range(tiles):
                hs[p, j, :, g * 128 : (g + 1) * 128] = hid[
                    g // 2, j * trows : (j + 1) * trows, o : o + 128
                ]
    for j in range(tiles):
        cols[j, me] = hs[me // 2, j]
    lhs[:rows] = hid[xl]

    send_c = []
    for k in NEAREST:
        device, m = on_plane(k)
        send_c.append(send(hs.at[m // 2], cols.at[:, me], device))
    unit_rows(gone, 1, quarter // 64)
    for k in range(1, 4):
        load_b[k].wait()
        unit_rows(lax.rem(gone + k, 4), 0, quarter // 64)

    send_w.wait()
    for copy in send_h:
        copy.wait()
    emb = jnp.dot(lhs[...], w[...].reshape(half, width), preferred_element_type=F32)
    ret[...] = emb[rows:]
    ue[...] = emb[:rows]
    send_e = [
        send(ret.at[upper], er.at[upper], pair),
        send(ret.at[lower], er.at[lower], cut),
    ]
    for i in range(1, CHUNKS):
        send_b[i].start()
    for copy in send_e:
        copy.wait()
    embed = ue[...] + er[...]
    length = jnp.sqrt(jnp.sum(embed * embed, axis=1, keepdims=True) + 1e-06)
    lens[...] = length
    unit = embed / length
    ue[...] = unit
    unit_b = unit.astype(BF16)
    pairt[:rows] = unit_b
    for j in range(tiles):
        units[j, me] = unit_b[j * trows : (j + 1) * trows]

    def along(h, second, d):
        if (h == 0) != second:
            return {"z": lax.rem(z + d, 4)}
        return {"y": lax.rem(y + d, 4)}

    def source(h, d):
        if h == 0:
            return lax.rem(z + 4 - d, 4) * 4 + y
        return z * 4 + lax.rem(y + 4 - d, 4)

    steps = (1, 3, 2)

    def gather(block):
        first, second = {}, []
        for d in steps:
            for h in range(2):
                first[h, d] = send(block(h, me), block(h, me), along(h, False, d))
        for d in steps:
            for h in range(2):
                second.append(send(block(h, me), block(h, me), along(h, True, d)))

        def forward():
            for d in steps:
                for h in range(2):
                    first[h, d].wait()
                    m = source(h, d)
                    for e in steps:
                        second.append(send(block(h, m), block(h, m), along(h, True, e)))

        def done():
            for copy in second:
                copy.wait()

        return forward, done

    def gather_relay(block, size):
        first, second, last = {}, {}, []
        for d in steps:
            for h in range(2):
                first[h, d] = send(block(h, me, 0, size), block(h, me, 0, size), along(h, False, d))
        for e in (1, 3):
            for h in range(2):
                second[h, 0, e] = send(block(h, me, 0, size), block(h, me, 0, size), along(h, True, e))

        def forward():
            for d in steps:
                for h in range(2):
                    first[h, d].wait()
                    m = source(h, d)
                    for e in (1, 3):
                        second[h, d, e] = send(
                            block(h, m, 0, size), block(h, m, 0, size), along(h, True, e)
                        )

        def relay():
            for d in (0,) + steps:
                for e in (1, 3):
                    for h in range(2):
                        second[h, d, e].wait()
                        dz, dy = (d, e) if h == 0 else (e, d)
                        m = lax.rem(z + 4 - dz, 4) * 4 + lax.rem(y + 4 - dy, 4)
                        o = 0 if e == 1 else size // 2
                        half_block = block(h, m, o, size // 2)
                        last.append(send(half_block, half_block, along(h, True, e)))

        def done():
            for copy in last:
                copy.wait()

        return forward, relay, done

    def gather_units(j):
        return gather(lambda h, m: units.at[j, m, :, pl.ds(h * (width // 2), width // 2)])

    flows = [gather_units(0), gather_units(1)]

    def pass_on(i):
        send_b[i].wait()
        pass_core[i].start()
        pass_pair[i].start()

    def pass_again(i):
        pass_pair[i].wait()
        pass_last[i].start()

    def weigh(slot, j, order, first):
        u = units[j].reshape(tile, width)
        total = None if first else acc[j].reshape(tile, width)
        for q in order:
            b = bu[slot, q]
            scores = lax.dot_general(u, b, (((1,), (1,)), ((), ())), preferred_element_type=F32)
            weight = jnp.exp(KERNEL_SCALE * scores).astype(BF16)
            term = jnp.dot(weight, b, preferred_element_type=F32)
            total = term if total is None else total + term
        acc[j] = total.reshape(4, 4, trows, width)

    batch = 2 * tiles * tile

    def near(j):
        u = units[j].reshape(tile, width)
        t = pairt[...]
        scores = lax.dot_general(u, t, (((1,), (1,)), ((), ())), preferred_element_type=F32)
        row = lax.broadcasted_iota(jnp.int32, scores.shape, 0) - me * trows
        column = lax.broadcasted_iota(jnp.int32, scores.shape, 1) - j * trows
        same = jnp.logical_and(row == column, jnp.logical_and(column >= 0, column < trows))
        weight = jnp.where(same, F32(0.0), jnp.exp(KERNEL_SCALE * scores)).astype(BF16)
        total = jnp.dot(weight, t, preferred_element_type=F32)
        less = total * (brows * 32 / (batch - 1))
        acc[j] = acc[j] - less.reshape(4, 4, trows, width)

    def finish(j):
        proof = acc[j] * (-1.0 / (brows * 32))
        acc[j] = proof
        wide[j] = proof.astype(BF16)
        sends = {}
        for d in steps:
            tz, ty = lax.rem(z + d, 4), lax.rem(y + d, 4)
            sends[0, d] = send(wide.at[j, tz, :, :, left], landed.at[j, 0, d - 1], {"z": tz})
            sends[1, d] = send(wide.at[j, :, ty, :, right], landed.at[j, 1, d - 1], {"y": ty})
        return sends

    left, right = pl.ds(0, width // 2), pl.ds(width // 2, width // 2)

    def middle(j, firsts):
        sends = []
        for h in range(2):
            part_sum = acc[j, z, :, :, left] if h == 0 else acc[j, :, y, :, right]
            for d in steps:
                firsts[h, d].wait()
                part_sum = part_sum + landed[j, h, d - 1].astype(F32)
            keep[...] = part_sum
            mids[j, h] = part_sum.astype(BF16)
            acc[j, 0, h, :, left] = keep[y if h == 0 else z]
            for e in steps:
                to = lax.rem((y if h == 0 else z) + e, 4)
                sends.append(
                    send(mids.at[j, h, to], landed2.at[j, h, e - 1], {"y": to} if h == 0 else {"z": to})
                )
        return sends

    def land(j, sends):
        for copy in sends:
            copy.wait()
        halves = []
        for h in range(2):
            own_sum = acc[j, 0, h, :, left]
            for e in steps:
                own_sum = own_sum + landed2[j, h, e - 1].astype(F32)
            halves.append(own_sum)
        proof = jnp.concatenate(halves, axis=1)
        r = slice(j * trows, (j + 1) * trows)
        unit = ue[r, :]
        radial = jnp.sum(unit * proof, axis=1, keepdims=True)
        grads[j, me] = ((proof - unit * radial) / lens[r, :]).astype(BF16)
        if j == tiles - 1:
            return gather(lambda h, m: grads.at[j, m, :, pl.ds(h * (width // 2), width // 2)])
        return gather_relay(
            lambda h, m, o, n: grads.at[j, m, :, pl.ds(h * (width // 2) + o, n)], width // 2
        )

    own = (0, 1, 2, 3)
    core_q = xl * 2 + 1 - c
    late_q = (pair_q, (1 - xl) * 2 + 1 - c)
    pass_on(0)
    flows[0][0]()
    flows.append(gather_units(2))
    pass_on(1)
    flows[1][0]()
    flows.append(gather_units(3))
    pass_on(2)
    flows[0][1]()
    pass_on(3)
    weigh(0, 0, own, True)
    flows[2][0]()
    pass_on(4)
    pass_again(0)
    pass_again(1)
    flows[1][1]()
    weigh(0, 1, own, True)
    flows[3][0]()
    pass_again(2)
    flows[2][1]()
    weigh(0, 2, (0, 1), True)
    pass_on(5)
    weigh(0, 2, (2, 3), False)
    pass_on(6)
    pass_again(3)
    flows[3][1]()
    weigh(0, 3, (0, 1), True)
    pass_on(7)
    weigh(0, 3, (2, 3), False)
    send_m = send(pairt.at[pl.ds(0, rows)], pairt.at[pl.ds(rows, rows)], far_mate)
    pass_again(4)
    weigh(1, 2, (own_q,), False)
    weigh(1, 3, (own_q,), False)
    pass_again(5)
    weigh(1, 0, (own_q,), False)
    weigh(1, 1, (own_q,), False)
    for i in range(CHUNKS):
        pass_core[i].wait()
    pass_again(6)
    weigh(1, 0, (core_q,), False)
    weigh(1, 1, (core_q,), False)
    pass_again(7)
    weigh(1, 2, (core_q,), False)
    weigh(1, 3, (core_q,), False)
    send_m.wait()
    for j in range(tiles):
        near(j)
    for i in range(CHUNKS):
        pass_last[i].wait()
    weigh(1, 0, late_q, False)
    send_p = [finish(0)]
    weigh(1, 1, late_q, False)
    send_p.append(finish(1))
    weigh(1, 2, late_q, False)
    send_p.append(finish(2))
    middles = [middle(0, send_p[0])]
    weigh(1, 3, late_q, False)
    send_p.append(finish(3))
    middles.append(middle(1, send_p[1]))
    spread = [land(0, middles[0])]
    middles.append(middle(2, send_p[2]))
    spread.append(land(1, middles[1]))
    middles.append(middle(3, send_p[3]))
    spread[0][0]()
    spread.append(land(2, middles[2]))
    spread[1][0]()
    spread[0][1]()
    spread.append(land(3, middles[3]))
    spread[2][0]()
    spread[1][1]()
    spread[3][0]()
    spread[2][1]()
    for copy in send_c:
        copy.wait()
    for j in range(tiles):
        spread[j][-1]()

    feats = cols[...].reshape(N_PLANE * rows, 512).T
    lane = lax.rem(y, 2) * 64

    def strip_of(axl, ac):
        return pl.ds(pl.multiple_of((axl * 2 + ac) * 128 + lane, 64), 64)

    swap = []
    for side in (left, right):
        samples_grads = grads[:, :, :, side].reshape(N_PLANE * rows, width // 2)
        part[:, side] = jnp.dot(feats, samples_grads, preferred_element_type=F32)
        swap.append([send(part.at[strip_of(a, 1 - c), side], mine.at[a, :, side], core) for a in range(2)])
    here = pl.ds(pl.multiple_of(xh * 32, 32), 32)
    send_x = []
    for h, side in enumerate((left, right)):
        for a in range(2):
            swap[h][a].wait()
            total = mine[a, :, side] + part[strip_of(a, c), side]
            mine[a, :, side] = total
            xout[h, a] = total.astype(BF16)
        for k in (1, 5, 4):
            to = on_line(k)
            block = xout.at[h, to["xl"], pl.ds(pl.multiple_of(to["xh"] * 32, 32), 32)]
            send_x.append(send(block, xin.at[len(send_x)], to))
    fold = jnp.zeros((8, 128), F32)
    for h, side in enumerate((left, right)):
        total = mine[xl, here, side]
        for i in range(3):
            send_x[h * 3 + i].wait()
            total = total + xin[h * 3 + i].astype(F32)
        grad[:, side] = total
        squares = total * total
        for a in range(4):
            for b in range(width // 256):
                fold = fold + squares[a * 8 : a * 8 + 8, b * 128 : b * 128 + 128]
    q1[...] = fold
    send_q = []
    for k in range(1, 8):
        send_q.append(send(q1, q1in.at[k - 1], on_line(k)))
    for k in range(1, 8):
        send_q[k - 1].wait()
        fold = fold + q1in[k - 1]
    q2[...] = fold
    send_q = []
    for k in range(1, N_PLANE):
        send_q.append(send(q2, q2in.at[k - 1], on_plane(k)[0]))
    for k in range(1, N_PLANE):
        send_q[k - 1].wait()
        fold = fold + q2in[k - 1]
    mean = jnp.sum(jnp.sum(fold, axis=1, keepdims=True), axis=0, keepdims=True) / (
        4 * strip * width
    )
    factor[...] = jnp.broadcast_to(lax.rsqrt(mean + 1e-06), factor.shape)


def local(latents, shift, scale_mod, head_weight, bank):
    rows, depth = latents.shape
    width = head_weight.shape[1]
    brows = bank.shape[0]
    vmem = pl.BlockSpec(memory_space=pltpu.VMEM)
    hbm = pl.BlockSpec(memory_space=pl.ANY)
    n_sems = 5 + 4 * CHUNKS + 15 + 4 * 30 + 1 + 4 * 12 + 3 * 38 + 30 + 10 + 7 + 15
    gradient, factor = pl.pallas_call(
        kernel,
        out_shape=(
            jax.ShapeDtypeStruct((depth // 128, width), F32),
            jax.ShapeDtypeStruct((1, 128), F32),
        ),
        in_specs=[hbm] * 5,
        out_specs=(vmem, vmem),
        scratch_shapes=[
            pltpu.VMEM((rows, depth), BF16),
            pltpu.VMEM((rows, depth), BF16),
            pltpu.VMEM((rows, depth), BF16),
            pltpu.VMEM((2, rows, depth // 2), BF16),
            pltpu.VMEM((2 * rows, depth // 2), BF16),
            pltpu.VMEM((2, depth // 4, width), BF16),
            pltpu.VMEM((rows, width), F32),
            pltpu.VMEM((rows, width), F32),
            pltpu.VMEM((rows, width), F32),
            pltpu.VMEM((rows, 1), F32),
            pltpu.VMEM((4, N_PLANE, rows // 4, width), BF16),
            pltpu.VMEM((2 * rows, width), BF16),
            pltpu.VMEM((2, 4, brows // 4, width), BF16),
            pltpu.VMEM((4, 4, 4, rows // 4, width), F32),
            pltpu.VMEM((4, 4, 4, rows // 4, width), BF16),
            pltpu.VMEM((4, 2, 3, 4, rows // 4, width // 2), BF16),
            pltpu.VMEM((4, 2, 4, rows // 4, width // 2), BF16),
            pltpu.VMEM((4, 2, 3, rows // 4, width // 2), BF16),
            pltpu.VMEM((4, rows // 4, width // 2), F32),
            pltpu.VMEM((N_PLANE // 2, 4, rows // 4, 512), BF16),
            pltpu.VMEM((4, N_PLANE, rows // 4, 512), BF16),
            pltpu.VMEM((4, N_PLANE, rows // 4, width), BF16),
            pltpu.VMEM((512, width), F32),
            pltpu.VMEM((2, 64, width), F32),
            pltpu.VMEM((6, 32, width // 2), BF16),
            pltpu.VMEM((2, 2, 64, width // 2), BF16),
            pltpu.VMEM((8, 128), F32),
            pltpu.VMEM((7, 8, 128), F32),
            pltpu.VMEM((8, 128), F32),
            pltpu.VMEM((15, 8, 128), F32),
            pltpu.SemaphoreType.DMA((17,)),
            pltpu.SemaphoreType.DMA((n_sems,)),
            pltpu.SemaphoreType.DMA((n_sems,)),
        ],
        compiler_params=pltpu.CompilerParams(
            collective_id=0, has_side_effects=True, vmem_limit_bytes=60 * 1024 * 1024
        ),
        name="mmd_step",
    )(latents, shift, scale_mod, head_weight, bank)
    return gradient * factor[0, 0]


def solution(mesh):
    torus = Mesh(mesh.devices.reshape(2, 2, 4, 4, 2), AXES)
    return jax.shard_map(
        local,
        mesh=torus,
        in_specs=(P(AXES, None), P(AXES, None), P(AXES, None), P(("xl", "c"), None), P(("z", "y", "xh"), None)),
        out_specs=P(AXES, None),
        check_vma=False,
    )
```
